128 devices in a mesh: grp: 8 (over z, core), brick: 16 (over x, y).
Axes of the slice: x: 4, y: 4, z: 4, core: 2. Of those that a mesh axis runs over, the one named last changes fastest.
Arguments:
- noisy: float32 [128, 64, 4096], P(('grp', 'brick')), may hold values from -6 to 6
- neighbours: int32 [128, 6], P(('grp', 'brick')), may hold values from -1 to 127, as said below
- labels: int32 [8, 16], P('grp'), may hold values from 0 to 2
- conv_in: float32 [64, 1728], replicated, may hold values from -0.15625 to 0.15625
- bias_in: float32 [64], replicated, may hold values from -3 to 3
- down_fine: float32 [128, 64], replicated, may hold values from -0.75 to 0.75
- conv_mid: float32 [128, 3456], replicated, may hold values from -0.109375 to 0.109375
- bias_mid: float32 [128], replicated, may hold values from -3 to 3
- conv_res: float32 [128, 3456], replicated, may hold values from -0.109375 to 0.109375
- conv_dec: float32 [128, 3456], replicated, may hold values from -0.109375 to 0.109375
- down_mid: float32 [256, 128], replicated, may hold values from -0.5 to 0.5
- w_query: float32 [256, 256], replicated, may hold values from -0.375 to 0.375
- w_key: float32 [256, 256], replicated, may hold values from -0.375 to 0.375
- w_value: float32 [256, 256], replicated, may hold values from -0.375 to 0.375
- w_out: float32 [256, 256], replicated, may hold values from -0.375 to 0.375
- logit_scale: float32 [4], replicated, may hold values from 1 to 40, as said below
- up_mid: float32 [128, 256], replicated, may hold values from -0.375 to 0.375
- up_fine: float32 [64, 128], replicated, may hold values from -0.5 to 0.5
- conv_out: float32 [64, 1728], replicated, may hold values from -0.15625 to 0.15625
Outputs:
- noise_pred: float32 [128, 64, 4096], P(('grp', 'brick'))
The draws below stay inside these ranges and needn't reach their ends.
Inputs may be any that keep to these rules, and one draw needn't show every extreme that they name: `neighbours`: row i lists, for faces -x, +x, -y, +y, -z, +z, the brick whose position touches brick i there, or -1. Where row i names j at face f, row j names i at face f xor 1. Bricks are numbered in Morton order of their positions. `logit_scale`: positive factors.
All inputs are finite; a program needn't handle non-finite values.
Results may differ from the reference program's by a relative error of at most 0.0003.
Values sent between devices are 32-bit elements; how exact they have to be, the bound alone decides.
No kernel may reach another device: no remote copies, remote signals or barrier semaphores. Data moves between devices by JAX's collectives and lax.ppermute only.
A program may use at most 192 MiB of HBM per device.

```python
import math
import jax
import jax.numpy as jnp
from jax import lax

S = 16
C1 = 64
C2 = 128
C3 = 256
HEADS = 4
HDIM = 64
TOKB = 64
BRICKS = 128
GROUPS = 8
MEMBERS = 16


def draw_neighbours(key, part):
    cell_count = 2 * BRICKS
    bit_width = cell_count.bit_length() - 1
    top_dim = (bit_width - 1) % 3
    low_start = 0
    for bit_pos in range(top_dim, bit_width - 1, 3):
        low_start = low_start + (1 << bit_pos)
    half_count = BRICKS // 2
    low_pool = jax.random.permutation(jax.random.fold_in(key, 11), BRICKS - low_start - 1).astype(jnp.int32)
    high_pool = jax.random.permutation(jax.random.fold_in(key, 13), BRICKS - 1).astype(jnp.int32)
    low_codes = jnp.concatenate([jnp.full((1,), low_start, jnp.int32), low_pool[:half_count - 1] + low_start + 1])
    high_codes = jnp.concatenate([jnp.full((1,), BRICKS, jnp.int32), high_pool[:half_count - 1] + BRICKS + 1])
    morton_codes = jnp.sort(jnp.concatenate([low_codes, high_codes]))
    position = []
    for dim_id in range(3):
        amount = jnp.zeros((BRICKS,), jnp.int32)
        for bit_pos in range(dim_id, bit_width, 3):
            amount = amount + (morton_codes >> bit_pos & 1) * (1 << bit_pos // 3)
        position.append(amount)
    lookup = jnp.full((cell_count,), -1, jnp.int32).at[morton_codes].set(jnp.arange(BRICKS, dtype=jnp.int32))
    columns = []
    for face_id in range(6):
        axis_id = face_id // 2
        stride = 2 * (face_id % 2) - 1
        shifted = [position[dim_id] + (stride if dim_id == axis_id else 0) for dim_id in range(3)]
        inside = (shifted[0] >= 0) & (shifted[1] >= 0) & (shifted[2] >= 0)
        moved_code = jnp.zeros((BRICKS,), jnp.int32)
        for dim_id in range(3):
            for bit_pos in range(bit_width // 3 + 2):
                moved_code = moved_code + (jnp.maximum(shifted[dim_id], 0) >> bit_pos & 1) * (1 << 3 * bit_pos + dim_id)
        inside = inside & (moved_code < cell_count)
        located = lookup[jnp.clip(moved_code, 0, cell_count - 1)]
        columns.append(jnp.where(inside, located, -1))
    return jnp.stack(columns, axis=1).astype(jnp.int32)


def draw_logit_scale(key, part):
    return jnp.exp(jax.random.uniform(key, (HEADS,), jnp.float32, 0.0, math.log(8.0)))


def touch_ends(result, own_key, smallest, top_value):
    index_at = [jax.random.randint(jax.random.fold_in(own_key, axis), (), 0, length) for axis, length in enumerate(result.shape)]
    widest = result.shape.index(max(result.shape))
    neighbour = index_at[:widest] + [(index_at[widest] + 1) % result.shape[widest]] + index_at[widest + 1:]
    return result.at[tuple(index_at)].set(smallest).at[tuple(neighbour)].set(top_value)


def levels(rng, dims, cuts, smallest, high):
    level = 1.0
    for dim, parts in cuts:
        steps = jax.random.uniform(jax.random.fold_in(jax.random.fold_in(rng, 6), dim), (parts,), jnp.float32, smallest / len(cuts), high / len(cuts))
        level = level * jnp.repeat(jnp.exp(steps), dims[dim] // parts).reshape((-1,) + (1,) * (len(dims) - 1 - dim))
    return level


def centred(stream_key, dims, deviation, reach, split=(), kind=jnp.bfloat16):
    loudness = levels(stream_key, dims, split, -0.22, 0.18) if split else 1.0
    entries = jax.random.normal(stream_key, dims, jnp.float32) * deviation * loudness
    return jnp.minimum(jnp.maximum(entries, -reach), reach).astype(kind)


def setup_inputs(seed: int = 0) -> dict:
    streams_of = jax.random.split(jax.random.key(seed), 20)
    return {
        "noisy": centred(streams_of[0], (BRICKS, C1, S ** 3), 1.0, 6.0, ((0, 128),), jnp.float32),
        "neighbours": draw_neighbours(jax.random.fold_in(streams_of[19], 71), 0),
        "labels": touch_ends(jax.random.randint(streams_of[2], (GROUPS, MEMBERS), 0, 3), jax.random.fold_in(streams_of[2], 1), 0, 2).astype(jnp.int32),
        "conv_in": centred(streams_of[3], (C1, 27 * C1), (27 * C1) ** -0.5, 0.15625, (), jnp.float32),
        "bias_in": centred(streams_of[4], (C1,), 0.5, 3.0, (), jnp.float32),
        "down_fine": centred(streams_of[5], (C2, C1), C1 ** -0.5, 0.75, (), jnp.float32),
        "conv_mid": centred(streams_of[6], (C2, 27 * C2), (27 * C2) ** -0.5, 0.109375, (), jnp.float32),
        "bias_mid": centred(streams_of[7], (C2,), 0.5, 3.0, (), jnp.float32),
        "conv_res": centred(streams_of[8], (C2, 27 * C2), (27 * C2) ** -0.5, 0.109375, (), jnp.float32),
        "conv_dec": centred(streams_of[9], (C2, 27 * C2), (27 * C2) ** -0.5, 0.109375, (), jnp.float32),
        "down_mid": centred(streams_of[10], (C3, C2), C2 ** -0.5, 0.5, (), jnp.float32),
        "w_query": centred(streams_of[11], (C3, C3), C3 ** -0.5, 0.375, (), jnp.float32),
        "w_key": centred(streams_of[12], (C3, C3), C3 ** -0.5, 0.375, (), jnp.float32),
        "w_value": centred(streams_of[13], (C3, C3), C3 ** -0.5, 0.375, (), jnp.float32),
        "w_out": centred(streams_of[14], (C3, C3), C3 ** -0.5, 0.375, (), jnp.float32),
        "logit_scale": draw_logit_scale(jax.random.fold_in(streams_of[19], 71), 0),
        "up_mid": centred(streams_of[16], (C2, C3), C3 ** -0.5, 0.375, (), jnp.float32),
        "up_fine": centred(streams_of[17], (C1, C2), C2 ** -0.5, 0.5, (), jnp.float32),
        "conv_out": centred(streams_of[18], (C1, 27 * C1), (27 * C1) ** -0.5, 0.15625, (), jnp.float32),
    }


HIGHEST = lax.Precision.HIGHEST
EPSILON = 1e-06

def face_layers(brick_block):
    channels = brick_block.shape[0]
    edge_len = brick_block.shape[1]
    sheets = [brick_block[:, 0], brick_block[:, -1], brick_block[:, :, 0], brick_block[:, :, -1], brick_block[:, :, :, 0], brick_block[:, :, :, -1]]
    return jnp.stack([one_sheet.reshape(channels, edge_len * edge_len) for one_sheet in sheets])

def padded_block(brick_block, halo_faces):
    channels = brick_block.shape[0]
    edge_len = brick_block.shape[1]
    sheets = halo_faces.reshape(6, channels, edge_len, edge_len)
    padded = jnp.pad(brick_block, ((0, 0), (1, 1), (1, 1), (1, 1)))
    padded = padded.at[:, 0, 1:-1, 1:-1].set(sheets[0])
    padded = padded.at[:, -1, 1:-1, 1:-1].set(sheets[1])
    padded = padded.at[:, 1:-1, 0, 1:-1].set(sheets[2])
    padded = padded.at[:, 1:-1, -1, 1:-1].set(sheets[3])
    padded = padded.at[:, 1:-1, 1:-1, 0].set(sheets[4])
    padded = padded.at[:, 1:-1, 1:-1, -1].set(sheets[5])
    return padded

def convolve(padded, weight):
    channels = padded.shape[0]
    edge_len = padded.shape[1] - 2
    voxels = edge_len ** 3
    summed = jnp.zeros((weight.shape[0], voxels), jnp.float32)
    for along_x in range(3):
        shifted = [padded[:, along_x:along_x + edge_len, along_y:along_y + edge_len, along_z:along_z + edge_len].reshape(channels, voxels) for along_y in range(3) for along_z in range(3)]
        stacked = jnp.concatenate(shifted, axis=0)
        weight_part = weight[:, along_x * 9 * channels:(along_x + 1) * 9 * channels]
        summed = summed + jnp.dot(weight_part, stacked, precision=HIGHEST, preferred_element_type=jnp.float32)
    return summed

def pooled(brick_block):
    channels = brick_block.shape[0]
    halved = brick_block.shape[1] // 2
    return brick_block.reshape(channels, halved, 2, halved, 2, halved, 2).mean(axis=(2, 4, 6))

def widened(brick_block):
    channels = brick_block.shape[0]
    edge_len = brick_block.shape[1]
    spread = jnp.broadcast_to(brick_block[:, :, None, :, None, :, None], (channels, edge_len, 2, edge_len, 2, edge_len, 2))
    return spread.reshape(channels, 2 * edge_len, 2 * edge_len, 2 * edge_len)

def head_norm(values):
    return values * lax.rsqrt(lax.optimization_barrier(jnp.mean(values * values, axis=-1, keepdims=True)) + EPSILON)

def level_conv(blocks, neighbours, weight):
    face_sheets = jax.vmap(face_layers)(blocks)
    opposite = jnp.array([1, 0, 3, 2, 5, 4], dtype=jnp.int32)
    clipped = jnp.clip(neighbours, 0, blocks.shape[0] - 1).astype(jnp.int32)
    picked = face_sheets[clipped, opposite[None, :]]
    halo_faces = jnp.where((neighbours >= 0)[:, :, None, None], picked, jnp.zeros_like(picked))
    return lax.map(lambda paired: convolve(padded_block(paired[0], paired[1]), weight), (blocks, halo_faces))

def attend(tokens, labels, w_query, w_key, w_value, w_out, logit_scale):
    brick_count = tokens.shape[0]
    groups = labels.shape[0]
    members = labels.shape[1]
    group_rows = members * TOKB
    normed = head_norm(tokens).reshape(brick_count * TOKB, C3)
    query_rows = head_norm(jnp.dot(normed, w_query, precision=HIGHEST).reshape(groups, group_rows, HEADS, HDIM))
    key_rows = head_norm(jnp.dot(normed, w_key, precision=HIGHEST).reshape(groups, group_rows, HEADS, HDIM))
    values = jnp.dot(normed, w_value, precision=HIGHEST).reshape(groups, group_rows, HEADS, HDIM)
    head_scale = logit_scale / jnp.sqrt(jnp.float32(HDIM))

    def one_group(packed):
        group_q, group_k, group_v, group_lab = packed
        token_lab = jnp.repeat(group_lab, TOKB)
        allowed = token_lab[:, None] == token_lab[None, :]
        logits = jnp.einsum('qhd,khd->hqk', group_q, group_k, precision=HIGHEST) * head_scale[:, None, None]
        logits = jnp.where(allowed[None], logits, -1e+30)
        row_peak = lax.optimization_barrier(jnp.max(logits, axis=-1, keepdims=True))
        exponent = jnp.where(allowed[None], jnp.exp(logits - row_peak), 0.0)
        weights = exponent / lax.optimization_barrier(jnp.sum(exponent, axis=-1, keepdims=True))
        return jnp.einsum('hqk,khd->qhd', weights, group_v, precision=HIGHEST).reshape(group_rows, C3)
    attended = lax.map(one_group, (query_rows, key_rows, values, labels)).reshape(brick_count * TOKB, C3)
    return tokens + jnp.dot(attended, w_out, precision=HIGHEST).reshape(brick_count, TOKB, C3)

def reference(noisy, neighbours, labels, conv_in, bias_in, down_fine, conv_mid, bias_mid, conv_res, conv_dec, down_mid, w_query, w_key, w_value, w_out, logit_scale, up_mid, up_fine, conv_out):
    brick_count = noisy.shape[0]
    half_edge = S // 2
    quarter = S // 4
    first_level = jax.nn.silu(level_conv(noisy.reshape(brick_count, C1, S, S, S), neighbours, conv_in) + bias_in[None, :, None])
    shrunk = jax.vmap(pooled)(first_level.reshape(brick_count, C1, S, S, S)).reshape(brick_count, C1, half_edge ** 3)
    mid_in = jnp.einsum('oc,bcv->bov', down_fine, shrunk, precision=HIGHEST)
    second = jax.nn.silu(level_conv(mid_in.reshape(brick_count, C2, half_edge, half_edge, half_edge), neighbours, conv_mid) + bias_mid[None, :, None])
    refined = second + jax.nn.silu(level_conv(second.reshape(brick_count, C2, half_edge, half_edge, half_edge), neighbours, conv_res))
    coarse = jax.vmap(pooled)(refined.reshape(brick_count, C2, half_edge, half_edge, half_edge)).reshape(brick_count, C2, TOKB)
    tokens = jnp.einsum('oc,bcv->bvo', down_mid, coarse, precision=HIGHEST)
    mixed = attend(tokens, labels, w_query, w_key, w_value, w_out, logit_scale)
    lifted = jnp.einsum('oc,bvc->bov', up_mid, mixed, precision=HIGHEST).reshape(brick_count, C2, quarter, quarter, quarter)
    joined = refined + jax.vmap(widened)(lifted).reshape(brick_count, C2, half_edge ** 3)
    decoded = jax.nn.silu(level_conv(joined.reshape(brick_count, C2, half_edge, half_edge, half_edge), neighbours, conv_dec))
    dropped = jnp.einsum('oc,bcv->bov', up_fine, decoded, precision=HIGHEST).reshape(brick_count, C1, half_edge, half_edge, half_edge)
    fine_mix = jax.nn.silu(first_level + jax.vmap(widened)(dropped).reshape(brick_count, C1, S ** 3))
    return level_conv(fine_mix.reshape(brick_count, C1, S, S, S), neighbours, conv_out).reshape(brick_count, C1, S ** 3)
```

```python
import jax
import jax.numpy as jnp
from jax import lax
from jax.experimental import pallas as pl
from jax.experimental.pallas import tpu as pltpu
from jax.sharding import PartitionSpec as P

S = 16
C1 = 64
C2 = 128
C3 = 256
HEADS = 4
HDIM = 64
TOKB = 64
BRICKS = 128
GROUPS = 8
MEMBERS = 16
SLOTS_B = 2
SLOTS_G = 3
FROM_B = 6
FROM_G = FROM_B + MEMBERS * SLOTS_B
FROM_X = FROM_G + GROUPS * SLOTS_G
EPSILON = 1e-06
ALL = ("grp", "brick")

f32 = jnp.float32
bf16 = jnp.bfloat16


def split(v):
    hi = v.astype(bf16)
    return hi, (v - hi.astype(f32)).astype(bf16)


def mm(a, b, nt=False):
    return lax.dot_general(
        a, b, (((1,), (1 if nt else 0,)), ((), ())), preferred_element_type=f32
    )


def dot3(a, b, nt=False):
    rows = a.shape[0]
    ah, al = split(a)
    bh, bl = split(b)
    both = mm(jnp.concatenate([ah, al], axis=0), bh, nt)
    return both[:rows] + both[rows:] + mm(ah, bl, nt)


def dot2(a, selector, nt=False):
    rows = a.shape[0]
    ah, al = split(a)
    both = mm(jnp.concatenate([ah, al], axis=0), selector, nt)
    return both[:rows] + both[rows:]


def iota(shape, dim):
    return lax.broadcasted_iota(jnp.int32, shape, dim)


def as01(mask):
    return jnp.where(mask, 1.0, 0.0).astype(bf16)


def silu(v):
    return v / (1.0 + jnp.exp(-v))


def lane_roll(v, shift):
    amount = shift % v.shape[1]
    return v if amount == 0 else pltpu.roll(v, amount, 1)


def in_range(index, edge):
    return (index >= 0) & (index < edge)


def face_taps(face):
    side = 2 * (face % 2)
    if face < 2:
        return [9 * side + 3 * a + b for a in range(3) for b in range(3)]
    if face < 4:
        return [9 * a + 3 * side + b for a in range(3) for b in range(3)]
    return [9 * a + 3 * b + side for a in range(3) for b in range(3)]


def tap_columns(w_ref, taps, channels):
    runs = []
    for t in taps:
        if runs and runs[-1][1] == t:
            runs[-1][1] = t + 1
        else:
            runs.append([t, t + 1])
    pieces = [w_ref[:, lo * channels : hi * channels] for lo, hi in runs]
    return pieces[0] if len(pieces) == 1 else jnp.concatenate(pieces, axis=1)


def coarse_edges():
    row = iota((384, 512), 0)
    col = iota((384, 512), 1)
    pair = row >> 7
    edge = ((row >> 6) & 1) * 7
    a = (row >> 3) & 7
    b = row & 7
    x = col >> 6
    y = (col >> 3) & 7
    z = col & 7
    along = jnp.where(pair == 0, x, jnp.where(pair == 1, y, z))
    first = jnp.where(pair == 0, y, x)
    last = jnp.where(pair == 2, y, z)
    return as01((along == edge) & (first == a) & (last == b))


def fine_sides():
    row = iota((256, 256), 0)
    col = iota((256, 256), 1)
    edge = (row >> 7) * 15
    return as01(((col & 15) == edge) & ((col >> 4) == (row & 15)))


def fine_sides_t():
    row = iota((256, 256), 0)
    col = iota((256, 256), 1)
    edge = (col >> 7) * 15
    return as01(((row & 15) == edge) & ((row >> 4) == (col & 15)))


def send_faces(faces_ref, send_ref, slot_ref, sems):
    def copy(face):
        return pltpu.make_async_copy(
            faces_ref.at[face], send_ref.at[slot_ref[face]], sems.at[face]
        )

    for face in range(6):

        @pl.when(slot_ref[face] >= 0)
        def _():
            copy(face).start()

    for face in range(6):

        @pl.when(slot_ref[face] >= 0)
        def _():
            copy(face).wait()


def fetch_halo(pools, bounds, index_ref, halo_ref, sems):
    def each(act):
        for face in range(6):
            source = index_ref[face]
            for pool, low, high in zip(pools, bounds[:-1], bounds[1:]):

                @pl.when((source >= low) & (source < high))
                def _():
                    copy = pltpu.make_async_copy(
                        pool.at[source - low], halo_ref.at[face], sems.at[face]
                    )
                    act(copy)

    each(lambda copy: copy.start())
    for face in range(6):

        @pl.when(index_ref[face] < 0)
        def _():
            halo_ref[face] = jnp.zeros(halo_ref.shape[1:], f32)

    each(lambda copy: copy.wait())


def coarse_faces(v, edges, faces_ref):
    rows = v.shape[0] // 2
    picked = dot2(v, edges, nt=True)
    low = iota((rows, 128), 1) < 64
    for pair in range(3):
        block = picked[:, pair * 128 : (pair + 1) * 128]
        top = block[:rows]
        bottom = block[rows:]
        faces_ref[2 * pair] = jnp.where(low, top, pltpu.roll(bottom, 64, 1))
        faces_ref[2 * pair + 1] = jnp.where(low, pltpu.roll(top, 64, 1), bottom)


def fine_faces(v_ref, faces_ref):
    faces_ref[0] = v_ref[:, 0:256]
    faces_ref[1] = v_ref[:, 3840:4096]
    sides = fine_sides_t()
    at_x = iota((C1, 128), 1) >> 4
    for half in range(2):
        found = [None] * 4
        for k in range(8):
            start = (half * 8 + k) * 256
            part = v_ref[:, start : start + 256]
            near = dot2(part, sides)
            new = [
                lane_roll(part[:, :128], 16 * k),
                lane_roll(part[:, 128:], 16 * k - 112),
                near[:, :128],
                near[:, 128:],
            ]
            if k == 0:
                found = new
            else:
                found = [jnp.where(at_x == k, n, o) for n, o in zip(new, found)]
        for kind in range(4):
            faces_ref[2 + kind, :, half * 128 : (half + 1) * 128] = found[kind]


def route_kernel(table_ref, me_ref, slot_ref, relay_ref, final_ref):
    g = me_ref[0]
    b = me_ref[1]
    me = g * MEMBERS + b

    def rank_b(i, face, member):
        count = jnp.int32(0)
        for other in range(5):
            j = table_ref[i * 6 + other]
            hit = (j >= 0) & ((j & 15) == member) & (other < face)
            count = count + jnp.where(hit, 1, 0)
        return count

    def rank_g(j, face, group):
        count = jnp.int32(0)
        for other in range(face):
            i = table_ref[j * 6 + other]
            hit = (i >= 0) & ((i >> 4) == group)
            count = count + jnp.where(hit, 1, 0)
        return count

    for face in range(6):
        j = table_ref[me * 6 + face]
        member = j & 15
        rank = rank_b(me, face, member)
        fine = (j >= 0) & (member != b) & (rank < SLOTS_B)
        slot_ref[face] = jnp.where(fine, member * SLOTS_B + rank, -1)
    for slot in range(GROUPS * SLOTS_G):
        relay_ref[slot] = jnp.int32(-1)

    def relay_to(group, carry):
        j = group * MEMBERS + b
        for face in range(6):
            i = table_ref[j * 6 + face]
            mine = (i >= 0) & ((i >> 4) == g) & (group != g)
            safe = jnp.maximum(i, 0)
            rank = rank_g(j, face, g)
            first = rank_b(safe, face ^ 1, b)
            member = safe & 15
            source = jnp.where(
                member == b, face ^ 1, FROM_B + member * SLOTS_B + first
            )
            fits = mine & (rank < SLOTS_G) & ((member == b) | (first < SLOTS_B))

            @pl.when(fits)
            def _():
                relay_ref[group * SLOTS_G + rank] = source

        return carry

    lax.fori_loop(0, GROUPS, relay_to, 0)
    for face in range(6):
        i = table_ref[me * 6 + face]
        safe = jnp.maximum(i, 0)
        first = jnp.minimum(rank_b(safe, face ^ 1, b), SLOTS_B - 1)
        group = safe >> 4
        rank = jnp.minimum(rank_g(me, face, group), SLOTS_G - 1)
        source = jnp.where(
            group == g,
            FROM_B + (safe & 15) * SLOTS_B + first,
            FROM_G + group * SLOTS_G + rank,
        )
        final_ref[face] = jnp.where(i >= 0, source, -1)


def relay_kernel(faces_ref, recv_ref, index_ref, out_ref, sems):
    def each(act):
        def one(slot, carry):
            source = index_ref[slot]

            @pl.when((source >= 0) & (source < FROM_B))
            def _():
                act(pltpu.make_async_copy(faces_ref.at[source], out_ref.at[slot], sems.at[slot]))

            @pl.when(source >= FROM_B)
            def _():
                act(
                    pltpu.make_async_copy(
                        recv_ref.at[source - FROM_B], out_ref.at[slot], sems.at[slot]
                    )
                )

            return carry

        lax.fori_loop(0, GROUPS * SLOTS_G, one, 0)

    each(lambda copy: copy.start())
    each(lambda copy: copy.wait())


def fine_face_kernel(v_ref, faces_ref):
    fine_faces(v_ref, faces_ref)


def pack_kernel(faces_ref, slot_ref, send_ref, sems):
    send_faces(faces_ref, send_ref, slot_ref, sems)


def split_weights(w_ref, stacked_ref):
    rows = w_ref.shape[0]
    hi, lo = split(w_ref[...])
    stacked_ref[0:rows, :] = hi
    stacked_ref[rows : 2 * rows, :] = lo


def fine_conv_kernel(v_ref, w_ref, out_ref, hi_ref, lo_ref, stacked_ref):
    split_weights(w_ref, stacked_ref)
    for ref in (hi_ref, lo_ref):
        ref[:, 0:256] = jnp.zeros((576, 256), bf16)
        ref[:, 4352:4608] = jnp.zeros((576, 256), bf16)
    lane = iota((C1, 256), 1)
    y = lane >> 4
    z = lane & 15

    def plane(x, carry):
        part = v_ref[:, pl.ds(pl.multiple_of(x * 256, 256), 256)]
        for tap in range(9):
            dy, dz = tap // 3 - 1, tap % 3 - 1
            moved = lane_roll(part, -(16 * dy + dz))
            keep = in_range(y + dy, S) & in_range(z + dz, S)
            hi, lo = split(jnp.where(keep, moved, 0.0))
            at = pl.ds(pl.multiple_of(x * 256 + 256, 256), 256)
            hi_ref[tap * C1 : (tap + 1) * C1, at] = hi
            lo_ref[tap * C1 : (tap + 1) * C1, at] = lo
        return carry

    lax.fori_loop(0, S, plane, 0)

    def block(n, carry):
        def gathered(ref):
            return jnp.concatenate(
                [
                    ref[:, pl.ds(pl.multiple_of(n * 512 + dx * 256, 256), 512)]
                    for dx in range(3)
                ],
                axis=0,
            )

        both = mm(stacked_ref[...], gathered(hi_ref))
        low = mm(stacked_ref[0:C1, :], gathered(lo_ref))
        at = pl.ds(pl.multiple_of(n * 512, 512), 512)
        out_ref[:, at] = both[:C1] + both[C1:] + low
        return carry

    lax.fori_loop(0, 8, block, 0)


def fine_halo(acc_ref, halo_ref, w_ref, out_ref):
    lane = iota((C1, 256), 1)
    a = lane >> 4
    b = lane & 15
    sheets = []
    for face in range(6):
        layer = halo_ref[face]
        his, los = [], []
        for tap in range(9):
            da, db = tap // 3 - 1, tap % 3 - 1
            keep = in_range(a + da, S) & in_range(b + db, S)
            moved = lane_roll(layer, -(16 * da + db))
            hi, lo = split(jnp.where(keep, moved, 0.0))
            his.append(hi)
            los.append(lo)
        wh, wl = split(tap_columns(w_ref, face_taps(face), C1))
        both = mm(jnp.concatenate([wh, wl], axis=0), jnp.concatenate(his, axis=0))
        low = mm(wh, jnp.concatenate(los, axis=0))
        sheets.append(both[:C1] + both[C1:] + low)
    sides = fine_sides()
    at_x = (iota((2 * C1, 256), 1) >> 4) & 7
    lane = iota((C1, 128), 1)
    for half in range(2):
        at = slice(half * 128, (half + 1) * 128)
        near = jnp.concatenate([sheets[4][:, at], sheets[5][:, at]], axis=1)
        hi, lo = split(near)
        spread = jnp.concatenate([hi, lo], axis=0)
        for k in range(8):
            x = half * 8 + k
            both = mm(spread * as01(at_x == k), sides)
            start = x * 256
            total = acc_ref[:, start : start + 256] + both[:C1] + both[C1:]
            low = lane_roll(sheets[2][:, at], -16 * k)
            high = lane_roll(sheets[3][:, at], 112 - 16 * k)
            ends = jnp.concatenate(
                [jnp.where(lane < 16, low, 0.0), jnp.where(lane >= 112, high, 0.0)], axis=1
            )
            total = total + ends
            if x == 0:
                total = total + sheets[0]
            if x == S - 1:
                total = total + sheets[1]
            out_ref[:, start : start + 256] = total


def fine_last_kernel(acc_ref, w_ref, recv_ref, relayed_ref, extra_ref, final_ref, out_ref, halo_ref, sems):
    fetch_halo(
        [recv_ref, relayed_ref, extra_ref], [FROM_B, FROM_G, FROM_X, FROM_X + 6], final_ref, halo_ref, sems
    )
    fine_halo(acc_ref, halo_ref, w_ref, out_ref)


def fine_first_kernel(
    acc_ref,
    w_ref,
    bias_ref,
    down_ref,
    recv_ref,
    relayed_ref,
    extra_ref,
    final_ref,
    links_ref,
    first_ref,
    mid_ref,
    send_ref,
    halo_ref,
    faces_ref,
    sems,
):
    fetch_halo(
        [recv_ref, relayed_ref, extra_ref], [FROM_B, FROM_G, FROM_X, FROM_X + 6], final_ref, halo_ref, sems
    )
    fine_halo(acc_ref, halo_ref, w_ref, first_ref)
    first_ref[...] = silu(first_ref[...] + bias_ref[...])
    row = iota((512, 128), 0)
    col = iota((512, 128), 1)
    target = (row >> 8) * 64 + ((row >> 5) & 7) * 8 + ((row >> 1) & 7)
    pool = jnp.where(target == col, 0.125, 0.0).astype(bf16)
    parts = []
    for quad in range(4):
        planes = [
            first_ref[:, (4 * quad + k) * 256 : (4 * quad + k + 1) * 256] for k in range(4)
        ]
        pair = jnp.concatenate([planes[0] + planes[1], planes[2] + planes[3]], axis=1)
        parts.append(dot2(pair, pool))
    shrunk = jnp.concatenate(parts, axis=1)
    mid_ref[...] = dot3(down_ref[...], shrunk)
    coarse_faces(shrunk, coarse_edges(), faces_ref)
    send_faces(faces_ref, send_ref, links_ref, sems)


def coarse_conv_kernel(v_ref, w_ref, out_ref, hi_ref, lo_ref, stacked_ref):
    split_weights(w_ref, stacked_ref)
    lane = iota((16, 512), 1)
    x = lane >> 6
    y = (lane >> 3) & 7
    z = lane & 7

    def chunk(n, carry):
        part = v_ref[pl.ds(pl.multiple_of(n * 16, 16), 16), :]
        for tap in range(27):
            dx, dy, dz = tap // 9 - 1, tap // 3 % 3 - 1, tap % 3 - 1
            keep = in_range(x + dx, 8) & in_range(y + dy, 8) & in_range(z + dz, 8)
            moved = lane_roll(part, -(64 * dx + 8 * dy + dz))
            hi, lo = split(jnp.where(keep, moved, 0.0))
            at = pl.ds(pl.multiple_of(tap * C2 + n * 16, 16), 16)
            hi_ref[at, :] = hi
            lo_ref[at, :] = lo
        return carry

    lax.fori_loop(0, C2 // 16, chunk, 0)

    def block(n, carry):
        at = pl.ds(pl.multiple_of(n * 256, 256), 256)
        both = mm(stacked_ref[...], hi_ref[:, at])
        low = mm(stacked_ref[0:C2, :], lo_ref[:, at])
        out_ref[:, at] = both[:C2] + both[C2:] + low
        return carry

    lax.fori_loop(0, 2, block, 0)


def coarse_halo(acc_ref, halo_ref, w_ref, edges, down=None):
    rows = halo_ref.shape[1]
    low_lane = iota((rows, 128), 1) < 64
    lane = iota((C2, 128), 1)
    a = (lane >> 3) & 7
    b = lane & 7
    sheets = []
    for pair in range(3):
        even = halo_ref[2 * pair]
        odd = halo_ref[2 * pair + 1]
        top = jnp.where(low_lane, even, pltpu.roll(odd, 64, 1))
        bottom = jnp.where(low_lane, pltpu.roll(even, 64, 1), odd)
        layer = jnp.concatenate([top, bottom], axis=0)
        if down is not None:
            layer = dot3(down, layer)
        his, los = [], []
        for tap in range(9):
            da, db = tap // 3 - 1, tap % 3 - 1
            keep = in_range(a + da, 8) & in_range(b + db, 8)
            moved = lane_roll(layer, -(8 * da + db))
            hi, lo = split(jnp.where(keep, moved, 0.0))
            his.append(hi)
            los.append(lo)
        eh, el = split(tap_columns(w_ref, face_taps(2 * pair), C2))
        oh, ol = split(tap_columns(w_ref, face_taps(2 * pair + 1), C2))
        both = mm(jnp.concatenate([eh, el, oh, ol], axis=0), jnp.concatenate(his, axis=0))
        low = mm(jnp.concatenate([eh, oh], axis=0), jnp.concatenate(los, axis=0))
        even_sum = both[0:C2] + both[C2 : 2 * C2] + low[0:C2]
        odd_sum = both[2 * C2 : 3 * C2] + both[3 * C2 :] + low[C2:]
        sheets.append(jnp.where(lane < 64, even_sum, odd_sum))
    return acc_ref[...] + dot2(jnp.concatenate(sheets, axis=1), edges)


def second_kernel(
    acc_ref,
    w_ref,
    bias_ref,
    down_ref,
    arrived_ref,
    links_ref,
    slot_ref,
    second_ref,
    faces_ref,
    send_ref,
    halo_ref,
    sems,
):
    fetch_halo([arrived_ref], [0, BRICKS], links_ref, halo_ref, sems)
    edges = coarse_edges()
    summed = coarse_halo(acc_ref, halo_ref, w_ref, edges, down_ref[...])
    second = silu(summed + bias_ref[...])
    second_ref[...] = second
    coarse_faces(second, edges, faces_ref)
    send_faces(faces_ref, send_ref, slot_ref, sems)


def pool_rows(scale):
    row = iota((64, 512), 0)
    col = iota((64, 512), 1)
    target = (col >> 7) * 16 + ((col >> 4) & 3) * 4 + ((col >> 1) & 3)
    return jnp.where(target == row, scale, 0.0).astype(bf16)


def refined_kernel(
    acc_ref,
    w_ref,
    second_ref,
    recv_ref,
    relayed_ref,
    extra_ref,
    final_ref,
    refined_ref,
    coarse_ref,
    halo_ref,
    sems,
):
    fetch_halo(
        [recv_ref, relayed_ref, extra_ref], [FROM_B, FROM_G, FROM_X, FROM_X + 6], final_ref, halo_ref, sems
    )
    summed = coarse_halo(acc_ref, halo_ref, w_ref, coarse_edges())
    refined = second_ref[...] + silu(summed)
    refined_ref[...] = refined
    pool = pool_rows(0.125)
    hi, lo = split(refined)
    coarse_ref[...] = mm(pool, hi, nt=True) + mm(pool, lo, nt=True)


def attention_kernel(
    all_ref,
    own_ref,
    refined_ref,
    down_ref,
    wq_ref,
    wk_ref,
    wv_ref,
    wo_ref,
    up_ref,
    scale_ref,
    labels_ref,
    me_ref,
    slot_ref,
    joined_ref,
    faces_ref,
    send_ref,
    sems,
):
    head_of = iota((C3, C3), 1) >> 6
    head_mean = jnp.where((iota((C3, C3), 0) >> 6) == head_of, 1.0 / HDIM, 0.0).astype(bf16)

    def normed(v):
        return v * lax.rsqrt(jnp.mean(v * v, axis=-1, keepdims=True) + EPSILON)

    def head_normed(v):
        return v * lax.rsqrt(dot2(v * v, head_mean) + EPSILON)

    tokens = dot3(own_ref[...], down_ref[...], nt=True)
    query = head_normed(dot3(normed(tokens), wq_ref[...]))
    everyone = normed(dot3(all_ref[...], down_ref[...], nt=True))
    keys = head_normed(dot3(everyone, wk_ref[...]))
    values = dot3(everyone, wv_ref[...])
    lane_head = iota((TOKB, C3), 1) >> 6
    stacked = jnp.concatenate(
        [
            jnp.where(lane_head == h, query, 0.0) * (scale_ref[h] * (HDIM**-0.5))
            for h in range(HEADS)
        ],
        axis=0,
    )
    logits = dot3(stacked, keys, nt=True)
    brick_of = iota((1, MEMBERS * TOKB), 1) >> 6
    key_label = jnp.zeros((1, MEMBERS * TOKB), jnp.int32)
    for member in range(MEMBERS):
        key_label = jnp.where(brick_of == member, labels_ref[member], key_label)
    allowed = key_label == labels_ref[me_ref[1]]
    logits = jnp.where(allowed, logits, -1e30)
    peak = jnp.max(logits, axis=-1, keepdims=True)
    weight = jnp.where(allowed, jnp.exp(logits - peak), 0.0)
    total = jnp.sum(weight, axis=-1, keepdims=True)
    heads = dot3(weight, values) / total
    attended = jnp.zeros((TOKB, C3), f32)
    for h in range(HEADS):
        attended = jnp.where(lane_head == h, heads[h * TOKB : (h + 1) * TOKB], attended)
    mixed = tokens + dot3(attended, wo_ref[...])
    lifted = dot3(up_ref[...], mixed, nt=True)
    joined = refined_ref[...] + dot2(lifted, pool_rows(1.0))
    joined_ref[...] = joined
    coarse_faces(joined, coarse_edges(), faces_ref)
    send_faces(faces_ref, send_ref, slot_ref, sems)


def decoded_kernel(
    acc_ref,
    w_ref,
    up_ref,
    first_ref,
    recv_ref,
    relayed_ref,
    extra_ref,
    final_ref,
    slot_ref,
    mix_ref,
    faces_ref,
    send_ref,
    halo_ref,
    sems,
):
    fetch_halo(
        [recv_ref, relayed_ref, extra_ref], [FROM_B, FROM_G, FROM_X, FROM_X + 6], final_ref, halo_ref, sems
    )
    decoded = silu(coarse_halo(acc_ref, halo_ref, w_ref, coarse_edges()))
    dropped = dot3(up_ref[...], decoded)
    row = iota((128, 1024), 0)
    col = iota((128, 1024), 1)
    source = (col >> 9) * 64 + ((col >> 5) & 7) * 8 + ((col >> 1) & 7)
    widen = as01(source == row)
    for quad in range(4):
        wide = dot2(dropped[:, quad * 128 : (quad + 1) * 128], widen)
        at = slice(quad * 1024, (quad + 1) * 1024)
        mix_ref[:, at] = silu(first_ref[:, at] + wide)
    fine_faces(mix_ref, faces_ref)
    send_faces(faces_ref, send_ref, slot_ref, sems)


VMEM = pl.BlockSpec(memory_space=pltpu.VMEM)
SMEM = pl.BlockSpec(memory_space=pltpu.SMEM)
HBM = pl.BlockSpec(memory_space=pl.ANY)


def call(kernel, outs, args=(), pools=(), scalars=(), scratch=(), far=0):
    near = len(outs) - far
    return pl.pallas_call(
        kernel,
        out_shape=[jax.ShapeDtypeStruct(o, f32) for o in outs],
        in_specs=[VMEM] * len(args) + [HBM] * len(pools) + [SMEM] * len(scalars),
        out_specs=[VMEM] * near + [HBM] * far,
        scratch_shapes=list(scratch),
    )(*args, *pools, *scalars)


def route(scalars, sizes):
    return pl.pallas_call(
        route_kernel,
        out_shape=[jax.ShapeDtypeStruct((n,), jnp.int32) for n in sizes],
        in_specs=[SMEM] * len(scalars),
        out_specs=[SMEM] * len(sizes),
    )(*scalars)


def copy_sems(count):
    return pltpu.SemaphoreType.DMA((count,))


def dense_halo(faces, links):
    owners = lax.broadcasted_iota(jnp.int32, (BRICKS, 6), 0)
    chosen = links[None, :] == owners
    parcel = jnp.zeros((BRICKS, *faces.shape[1:]), f32)
    for face in range(6):
        parcel = jnp.where(chosen[:, face, None, None], faces[face][None], parcel)
    arrived = lax.all_to_all(parcel, ALL, 0, 0, tiled=True)
    halos = []
    for face in range(6):
        layer = lax.dynamic_index_in_dim(
            arrived, jnp.maximum(links[face], 0), 0, keepdims=False
        )
        halos.append(jnp.where(links[face] >= 0, layer, 0.0))
    return jnp.stack(halos)


def exchange(faces, send, relay, links, spilled):
    layer = faces.shape[1:]
    recv = lax.all_to_all(send, "brick", 0, 0, tiled=True)
    (onward,) = call(
        relay_kernel,
        [(GROUPS * SLOTS_G, *layer)],
        pools=[faces, recv],
        scalars=[relay],
        scratch=[copy_sems(GROUPS * SLOTS_G)],
        far=1,
    )
    arrived = lax.all_to_all(onward, "grp", 0, 0, tiled=True)
    extra = lax.cond(
        spilled, lambda v: dense_halo(v, links), lambda v: v, faces
    )
    return [recv, arrived, extra]


def overflows(table):
    rows = table.T
    bricks = lax.iota(jnp.int32, BRICKS)
    spilled = jnp.zeros((BRICKS,), jnp.bool_)
    for face in range(6):
        here = rows[face]
        same_b = jnp.zeros((BRICKS,), jnp.int32)
        same_g = jnp.zeros((BRICKS,), jnp.int32)
        for other in range(face):
            there = rows[other]
            same_b += ((there >= 0) & ((there & 15) == (here & 15))).astype(jnp.int32)
            same_g += ((there >= 0) & ((there >> 4) == (here >> 4))).astype(jnp.int32)
        valid = here >= 0
        over_b = valid & ((here & 15) != (bricks & 15)) & (same_b >= SLOTS_B)
        over_g = valid & ((here >> 4) != (bricks >> 4)) & (same_g >= SLOTS_G)
        spilled = spilled | over_b | over_g
    return jnp.any(spilled)


def per_device(
    noisy,
    neighbours,
    labels,
    conv_in,
    bias_in,
    down_fine,
    conv_mid,
    bias_mid,
    conv_res,
    conv_dec,
    down_mid,
    w_query,
    w_key,
    w_value,
    w_out,
    logit_scale,
    up_mid,
    up_fine,
    conv_out,
):
    links = neighbours[0]
    me = jnp.stack([lax.axis_index("grp"), lax.axis_index("brick")]).astype(jnp.int32)
    row = jnp.pad(links, (0, 122))
    rows = lax.all_to_all(
        jnp.broadcast_to(row[None], (BRICKS, 128)), ALL, 0, 0, tiled=True
    )
    table = rows[:, :6]
    spilled = overflows(table)
    slot, relay, final = route(
        [table.reshape(-1), me], [6, GROUPS * SLOTS_G, 6]
    )
    everything = jnp.where(links >= 0, FROM_X + lax.iota(jnp.int32, 6), -1)
    final = jnp.where(spilled, everything, final)

    def swap(faces, send):
        return exchange(faces, send, relay, links, spilled)

    def halo_scratch(rows, lanes):
        return [pltpu.VMEM((6, rows, lanes), f32), copy_sems(6)]

    fine_layer = (6, C1, 256)
    fine_send = (MEMBERS * SLOTS_B, C1, 256)
    layer = (6, C2 // 2, 128)
    layer_send = (MEMBERS * SLOTS_B, C2 // 2, 128)

    def fine_conv(v, w):
        return call(
            fine_conv_kernel,
            [(C1, S**3)],
            [v, w],
            scratch=[
                pltpu.VMEM((576, 4608), bf16),
                pltpu.VMEM((576, 4608), bf16),
                pltpu.VMEM((2 * C1, 27 * C1), bf16),
            ],
        )[0]

    def coarse_conv(v, w):
        return call(
            coarse_conv_kernel,
            [(C2, 512)],
            [v, w],
            scratch=[
                pltpu.VMEM((27 * C2, 512), bf16),
                pltpu.VMEM((27 * C2, 512), bf16),
                pltpu.VMEM((2 * C2, 27 * C2), bf16),
            ],
        )[0]

    fine_in = noisy[0]
    (faces,) = call(fine_face_kernel, [fine_layer], [fine_in])
    (send,) = call(
        pack_kernel, [fine_send], [faces], scalars=[slot], scratch=[copy_sems(6)], far=1
    )
    acc = fine_conv(fine_in, conv_in)
    pools = swap(faces, send)
    first, mid, send = call(
        fine_first_kernel,
        [(C1, S**3), (C2, 512), (BRICKS, C1 // 2, 128)],
        [acc, conv_in, bias_in[:, None], down_fine],
        pools,
        [final, links],
        [pltpu.VMEM(fine_layer, f32), pltpu.VMEM((6, C1 // 2, 128), f32), copy_sems(6)],
        far=1,
    )
    acc = coarse_conv(mid, conv_mid)
    arrived = lax.all_to_all(send, ALL, 0, 0, tiled=True)
    second, faces, send = call(
        second_kernel,
        [(C2, 512), layer, layer_send],
        [acc, conv_mid, bias_mid[:, None], down_fine],
        [arrived],
        [links, slot],
        halo_scratch(C1 // 2, 128),
        far=1,
    )
    acc = coarse_conv(second, conv_res)
    pools = swap(faces, send)
    refined, coarse = call(
        refined_kernel,
        [(C2, 512), (TOKB, C2)],
        [acc, conv_res, second],
        pools,
        [final],
        halo_scratch(C2 // 2, 128),
    )
    everyone = lax.all_to_all(
        jnp.broadcast_to(coarse[None], (MEMBERS, TOKB, C2)), "brick", 0, 0, tiled=True
    )
    joined, faces, send = call(
        attention_kernel,
        [(C2, 512), layer, layer_send],
        [
            everyone.reshape(MEMBERS * TOKB, C2),
            coarse,
            refined,
            down_mid,
            w_query,
            w_key,
            w_value,
            w_out,
            up_mid,
        ],
        [],
        [logit_scale, labels[0], me, slot],
        [copy_sems(6)],
        far=1,
    )
    acc = coarse_conv(joined, conv_dec)
    pools = swap(faces, send)
    mix, faces, send = call(
        decoded_kernel,
        [(C1, S**3), fine_layer, fine_send],
        [acc, conv_dec, up_fine, first],
        pools,
        [final, slot],
        halo_scratch(C2 // 2, 128),
        far=1,
    )
    acc = fine_conv(mix, conv_out)
    pools = swap(faces, send)
    (result,) = call(
        fine_last_kernel,
        [(C1, S**3)],
        [acc, conv_out],
        pools,
        [final],
        halo_scratch(C1, 256),
    )
    return result[None]


def solution(mesh):
    in_specs = (
        P(("grp", "brick"), None, None),
        P(("grp", "brick"), None),
        P("grp", None),
    ) + (P(),) * 16
    out_specs = P(("grp", "brick"), None, None)
    return jax.shard_map(
        per_device, mesh=mesh, in_specs=in_specs, out_specs=out_specs, check_vma=False
    )
```

```python
import jax
import jax.numpy as jnp
from jax import lax
from jax.experimental import pallas as pl
from jax.experimental.pallas import tpu as pltpu
from jax.sharding import PartitionSpec as P

S = 16
C1 = 64
C2 = 128
C3 = 256
HEADS = 4
HDIM = 64
TOKB = 64
BRICKS = 128
GROUPS = 8
MEMBERS = 16
SLOTS_B = 2
SLOTS_G = 3
FROM_B = 6
FROM_X = FROM_B + MEMBERS * SLOTS_B
FROM_G = FROM_X + MEMBERS
FROM_END = FROM_G + GROUPS * SLOTS_G
EPSILON = 1e-06
ALL = ("grp", "brick")

f32 = jnp.float32
bf16 = jnp.bfloat16


def split(v):
    hi = v.astype(bf16)
    return hi, (v - hi.astype(f32)).astype(bf16)


def mm(a, b, nt=False):
    return lax.dot_general(
        a, b, (((1,), (1 if nt else 0,)), ((), ())), preferred_element_type=f32
    )


def dot3(a, b, nt=False):
    rows = a.shape[0]
    ah, al = split(a)
    bh, bl = split(b)
    both = mm(jnp.concatenate([ah, al], axis=0), bh, nt)
    return both[:rows] + both[rows:] + mm(ah, bl, nt)


def dot2(a, selector, nt=False):
    rows = a.shape[0]
    ah, al = split(a)
    both = mm(jnp.concatenate([ah, al], axis=0), selector, nt)
    return both[:rows] + both[rows:]


def iota(shape, dim):
    return lax.broadcasted_iota(jnp.int32, shape, dim)


def as01(mask):
    return jnp.where(mask, 1.0, 0.0).astype(bf16)


def silu(v):
    return v / (1.0 + jnp.exp(-v))


def lane_roll(v, shift):
    amount = shift % v.shape[1]
    return v if amount == 0 else pltpu.roll(v, amount, 1)


def in_range(index, edge):
    return (index >= 0) & (index < edge)


def face_taps(face):
    side = 2 * (face % 2)
    if face < 2:
        return [9 * side + 3 * a + b for a in range(3) for b in range(3)]
    if face < 4:
        return [9 * a + 3 * side + b for a in range(3) for b in range(3)]
    return [9 * a + 3 * b + side for a in range(3) for b in range(3)]


def tap_columns(w_ref, taps, channels):
    runs = []
    for t in taps:
        if runs and runs[-1][1] == t:
            runs[-1][1] = t + 1
        else:
            runs.append([t, t + 1])
    pieces = [w_ref[:, lo * channels : hi * channels] for lo, hi in runs]
    return pieces[0] if len(pieces) == 1 else jnp.concatenate(pieces, axis=1)


def coarse_edges():
    row = iota((384, 512), 0)
    col = iota((384, 512), 1)
    pair = row >> 7
    edge = ((row >> 6) & 1) * 7
    a = (row >> 3) & 7
    b = row & 7
    x = col >> 6
    y = (col >> 3) & 7
    z = col & 7
    along = jnp.where(pair == 0, x, jnp.where(pair == 1, y, z))
    first = jnp.where(pair == 0, y, x)
    last = jnp.where(pair == 2, y, z)
    return as01((along == edge) & (first == a) & (last == b))


def fine_sides():
    row = iota((256, 256), 0)
    col = iota((256, 256), 1)
    edge = (row >> 7) * 15
    return as01(((col & 15) == edge) & ((col >> 4) == (row & 15)))


def fine_sides_t():
    row = iota((256, 256), 0)
    col = iota((256, 256), 1)
    edge = (col >> 7) * 15
    return as01(((row & 15) == edge) & ((row >> 4) == (col & 15)))


class Late:
    def __init__(self, far_ref, near_ref, sem):
        self.near_ref = near_ref
        self.copy = pltpu.make_async_copy(far_ref, near_ref, sem)
        self.copy.start()
        self.here = False

    def __getitem__(self, index):
        if not self.here:
            self.copy.wait()
            self.here = True
        return self.near_ref[index]


def late_copies(far_refs, near_refs, sems):
    return [
        Late(far, near, sems.at[n]) for n, (far, near) in enumerate(zip(far_refs, near_refs))
    ]


def send_faces(faces_ref, slot_ref, send_refs, sems):
    def each(act):
        for face in range(6):
            slot = slot_ref[face]
            base = 0
            for send_ref in send_refs:
                count = send_ref.shape[0]
                inside = (slot >= base) & (slot < base + count)

                @pl.when(inside)
                def _():
                    act(
                        pltpu.make_async_copy(
                            faces_ref.at[face], send_ref.at[slot - base], sems.at[face]
                        )
                    )

                base += count

    each(lambda copy: copy.start())
    each(lambda copy: copy.wait())


def fetch_halo(pools, bounds, index_ref, halo_ref, sems):
    def each(act):
        for face in range(6):
            source = index_ref[face]
            for pool, low, high in zip(pools, bounds[:-1], bounds[1:]):

                @pl.when((source >= low) & (source < high))
                def _():
                    act(
                        pltpu.make_async_copy(
                            pool.at[source - low], halo_ref.at[face], sems.at[face]
                        )
                    )

    each(lambda copy: copy.start())
    for face in range(6):

        @pl.when(index_ref[face] < 0)
        def _():
            halo_ref[face] = jnp.zeros(halo_ref.shape[1:], f32)

    return lambda: each(lambda copy: copy.wait())


BOUNDS = [FROM_B, FROM_X, FROM_G, FROM_END]


def coarse_faces(v, edges, faces_ref):
    rows = v.shape[0] // 2
    picked = dot2(v, edges, nt=True)
    low = iota((rows, 128), 1) < 64
    for pair in range(3):
        block = picked[:, pair * 128 : (pair + 1) * 128]
        top = block[:rows]
        bottom = block[rows:]
        faces_ref[2 * pair] = jnp.where(low, top, pltpu.roll(bottom, 64, 1))
        faces_ref[2 * pair + 1] = jnp.where(low, pltpu.roll(top, 64, 1), bottom)


def fine_faces(v_ref, faces_ref):
    faces_ref[0] = v_ref[:, 0:256]
    faces_ref[1] = v_ref[:, 3840:4096]
    sides = fine_sides_t()
    at_x = iota((C1, 128), 1) >> 4
    for half in range(2):
        found = [None] * 4
        for k in range(8):
            start = (half * 8 + k) * 256
            part = v_ref[:, start : start + 256]
            near = dot2(part, sides)
            new = [
                lane_roll(part[:, :128], 16 * k),
                lane_roll(part[:, 128:], 16 * k - 112),
                near[:, :128],
                near[:, 128:],
            ]
            if k == 0:
                found = new
            else:
                found = [jnp.where(at_x == k, n, o) for n, o in zip(new, found)]
        for kind in range(4):
            faces_ref[2 + kind, :, half * 128 : (half + 1) * 128] = found[kind]


def route_kernel(all_ref, table_ref, me_ref, slot_ref, relay_ref, final_ref, level_ref):
    g = me_ref[0]
    b = me_ref[1]
    me = g * MEMBERS + b
    here = all_ref[...]
    brick = iota((BRICKS, 128), 0)
    same_b = jnp.zeros((BRICKS, 128), f32)
    same_g = jnp.zeros((BRICKS, 128), f32)
    for back in range(1, 6):
        there = pltpu.roll(here, back, 1)
        known = there >= 0
        same_b += jnp.where(known & ((there & 15) == (here & 15)), 1.0, 0.0)
        same_g += jnp.where(known & ((there >> 4) == (here >> 4)), 1.0, 0.0)
    same_b = jnp.where((here >= 0) & ((here & 15) != (brick & 15)), same_b, 0.0)
    same_g = jnp.where((here >= 0) & ((here >> 4) != (brick >> 4)), same_g, 0.0)
    most_b = jnp.max(same_b).astype(jnp.int32)
    most_g = jnp.max(same_g).astype(jnp.int32)
    crowded = (most_b > SLOTS_B) | (most_g >= SLOTS_G)
    level = jnp.where(crowded, 2, jnp.where(most_b == SLOTS_B, 1, 0))
    level_ref[0] = level

    def rank_b(i, face, member):
        count = jnp.int32(0)
        for other in range(5):
            j = table_ref[i, other]
            hit = (j >= 0) & ((j & 15) == member) & (other < face)
            count = count + jnp.where(hit, 1, 0)
        return count

    def rank_g(j, face, group):
        count = jnp.int32(0)
        for other in range(face):
            i = table_ref[j, other]
            hit = (i >= 0) & ((i >> 4) == group)
            count = count + jnp.where(hit, 1, 0)
        return count

    def slot_b(member, rank):
        low = member * SLOTS_B + jnp.minimum(rank, SLOTS_B - 1)
        return jnp.where(rank < SLOTS_B, low, MEMBERS * SLOTS_B + member)

    for face in range(6):
        j = table_ref[me, face]
        member = j & 15
        rank = rank_b(me, face, member)
        fine = (j >= 0) & (member != b) & (rank <= SLOTS_B)
        slot_ref[face] = jnp.where(fine, slot_b(member, rank), -1)
    for slot in range(GROUPS * SLOTS_G):
        relay_ref[slot] = jnp.int32(-1)

    def relay_to(group, carry):
        j = group * MEMBERS + b
        for face in range(6):
            i = table_ref[j, face]
            mine = (i >= 0) & ((i >> 4) == g) & (group != g)
            safe = jnp.maximum(i, 0)
            rank = rank_g(j, face, g)
            first = rank_b(safe, face ^ 1, b)
            member = safe & 15
            source = jnp.where(member == b, face ^ 1, FROM_B + slot_b(member, first))
            fits = mine & (rank < SLOTS_G) & ((member == b) | (first <= SLOTS_B))

            @pl.when(fits)
            def _():
                relay_ref[group * SLOTS_G + rank] = source

        return carry

    lax.fori_loop(0, GROUPS, relay_to, 0)
    for face in range(6):
        i = table_ref[me, face]
        safe = jnp.maximum(i, 0)
        first = rank_b(safe, face ^ 1, b)
        group = safe >> 4
        rank = jnp.minimum(rank_g(me, face, group), SLOTS_G - 1)
        source = jnp.where(
            group == g,
            FROM_B + slot_b(safe & 15, first),
            FROM_G + group * SLOTS_G + rank,
        )
        source = jnp.where(level == 2, FROM_X + face, source)
        final_ref[face] = jnp.where(i >= 0, source, -1)


def relay_kernel(faces_ref, recv_ref, more_ref, index_ref, out_ref, sems):
    def each(act):
        def one(slot, carry):
            source = index_ref[slot]
            starts = [0, FROM_B, FROM_X, FROM_G]
            for pool, low, high in zip(
                (faces_ref, recv_ref, more_ref), starts[:-1], starts[1:]
            ):

                @pl.when((source >= low) & (source < high))
                def _():
                    act(
                        pltpu.make_async_copy(
                            pool.at[source - low], out_ref.at[slot], sems.at[slot]
                        )
                    )

            return carry

        lax.fori_loop(0, GROUPS * SLOTS_G, one, 0)

    each(lambda copy: copy.start())
    each(lambda copy: copy.wait())


def fine_face_kernel(v_ref, faces_ref):
    fine_faces(v_ref, faces_ref)


def pack_kernel(faces_ref, slot_ref, send_ref, spill_ref, sems):
    send_faces(faces_ref, slot_ref, [send_ref, spill_ref], sems)


def split_weights(w_ref, stacked_ref):
    rows = w_ref.shape[0]
    hi, lo = split(w_ref[...])
    stacked_ref[0:rows, :] = hi
    stacked_ref[rows : 2 * rows, :] = lo


def fine_conv_kernel(v_ref, w_ref, out_ref, hi_ref, lo_ref, stacked_ref):
    split_weights(w_ref, stacked_ref)
    for ref in (hi_ref, lo_ref):
        ref[:, 0:256] = jnp.zeros((576, 256), bf16)
        ref[:, 4352:4608] = jnp.zeros((576, 256), bf16)
    lane = iota((C1, 256), 1)
    y = lane >> 4
    z = lane & 15

    def plane(x, carry):
        part = v_ref[:, pl.ds(pl.multiple_of(x * 256, 256), 256)]
        for tap in range(9):
            dy, dz = tap // 3 - 1, tap % 3 - 1
            moved = lane_roll(part, -(16 * dy + dz))
            keep = in_range(y + dy, S) & in_range(z + dz, S)
            hi, lo = split(jnp.where(keep, moved, 0.0))
            at = pl.ds(pl.multiple_of(x * 256 + 256, 256), 256)
            hi_ref[tap * C1 : (tap + 1) * C1, at] = hi
            lo_ref[tap * C1 : (tap + 1) * C1, at] = lo
        return carry

    lax.fori_loop(0, S, plane, 0)

    def block(n, carry):
        def gathered(ref):
            return jnp.concatenate(
                [
                    ref[:, pl.ds(pl.multiple_of(n * 512 + dx * 256, 256), 512)]
                    for dx in range(3)
                ],
                axis=0,
            )

        both = mm(stacked_ref[...], gathered(hi_ref))
        low = mm(stacked_ref[0:C1, :], gathered(lo_ref))
        at = pl.ds(pl.multiple_of(n * 512, 512), 512)
        out_ref[:, at] = both[:C1] + both[C1:] + low
        return carry

    lax.fori_loop(0, 8, block, 0)


def fine_halo(acc_ref, halo_ref, w_ref, out_ref):
    lane = iota((C1, 256), 1)
    a = lane >> 4
    b = lane & 15
    sheets = []
    for face in range(6):
        layer = halo_ref[face]
        his, los = [], []
        for tap in range(9):
            da, db = tap // 3 - 1, tap % 3 - 1
            keep = in_range(a + da, S) & in_range(b + db, S)
            moved = lane_roll(layer, -(16 * da + db))
            hi, lo = split(jnp.where(keep, moved, 0.0))
            his.append(hi)
            los.append(lo)
        wh, wl = split(tap_columns(w_ref, face_taps(face), C1))
        both = mm(jnp.concatenate([wh, wl], axis=0), jnp.concatenate(his, axis=0))
        low = mm(wh, jnp.concatenate(los, axis=0))
        sheets.append(both[:C1] + both[C1:] + low)
    sides = fine_sides()
    at_x = (iota((2 * C1, 256), 1) >> 4) & 7
    lane = iota((C1, 128), 1)
    for half in range(2):
        at = slice(half * 128, (half + 1) * 128)
        near = jnp.concatenate([sheets[4][:, at], sheets[5][:, at]], axis=1)
        hi, lo = split(near)
        spread = jnp.concatenate([hi, lo], axis=0)
        for k in range(8):
            x = half * 8 + k
            both = mm(spread * as01(at_x == k), sides)
            start = x * 256
            total = acc_ref[:, start : start + 256] + both[:C1] + both[C1:]
            low = lane_roll(sheets[2][:, at], -16 * k)
            high = lane_roll(sheets[3][:, at], 112 - 16 * k)
            ends = jnp.concatenate(
                [jnp.where(lane < 16, low, 0.0), jnp.where(lane >= 112, high, 0.0)], axis=1
            )
            total = total + ends
            if x == 0:
                total = total + sheets[0]
            if x == S - 1:
                total = total + sheets[1]
            out_ref[:, start : start + 256] = total


def fine_last_kernel(
    recv_ref,
    more_ref,
    relayed_ref,
    acc_far,
    w_far,
    final_ref,
    out_ref,
    halo_ref,
    acc_near,
    w_near,
    sems,
    halo_sems,
):
    arrive = fetch_halo([recv_ref, more_ref, relayed_ref], BOUNDS, final_ref, halo_ref, halo_sems)
    acc_ref, w_ref = late_copies([acc_far, w_far], [acc_near, w_near], sems)
    arrive()
    fine_halo(acc_ref, halo_ref, w_ref, out_ref)


def fine_first_kernel(
    bias_ref,
    down_ref,
    recv_ref,
    more_ref,
    relayed_ref,
    acc_far,
    w_far,
    final_ref,
    links_ref,
    mid_ref,
    first_far,
    send_ref,
    halo_ref,
    first_ref,
    faces_ref,
    acc_near,
    w_near,
    sems,
    halo_sems,
    send_sems,
):
    arrive = fetch_halo([recv_ref, more_ref, relayed_ref], BOUNDS, final_ref, halo_ref, halo_sems)
    acc_ref, w_ref = late_copies([acc_far, w_far], [acc_near, w_near], sems)
    arrive()
    fine_halo(acc_ref, halo_ref, w_ref, first_ref)
    first_ref[...] = silu(first_ref[...] + bias_ref[...])
    keep = pltpu.make_async_copy(first_ref, first_far, sems.at[0])
    keep.start()
    row = iota((512, 128), 0)
    col = iota((512, 128), 1)
    target = (row >> 8) * 64 + ((row >> 5) & 7) * 8 + ((row >> 1) & 7)
    pool = jnp.where(target == col, 0.125, 0.0).astype(bf16)
    parts = []
    for quad in range(4):
        planes = [
            first_ref[:, (4 * quad + k) * 256 : (4 * quad + k + 1) * 256] for k in range(4)
        ]
        pair = jnp.concatenate([planes[0] + planes[1], planes[2] + planes[3]], axis=1)
        parts.append(dot2(pair, pool))
    shrunk = jnp.concatenate(parts, axis=1)
    mid_ref[...] = dot3(down_ref[...], shrunk)
    coarse_faces(shrunk, coarse_edges(), faces_ref)
    send_faces(faces_ref, links_ref, [send_ref], send_sems)
    keep.wait()


def coarse_conv_kernel(v_ref, w_ref, out_ref, hi_ref, lo_ref, stacked_ref):
    split_weights(w_ref, stacked_ref)
    lane = iota((16, 512), 1)
    x = lane >> 6
    y = (lane >> 3) & 7
    z = lane & 7

    def chunk(n, carry):
        part = v_ref[pl.ds(pl.multiple_of(n * 16, 16), 16), :]
        for tap in range(27):
            dx, dy, dz = tap // 9 - 1, tap // 3 % 3 - 1, tap % 3 - 1
            keep = in_range(x + dx, 8) & in_range(y + dy, 8) & in_range(z + dz, 8)
            moved = lane_roll(part, -(64 * dx + 8 * dy + dz))
            hi, lo = split(jnp.where(keep, moved, 0.0))
            at = pl.ds(pl.multiple_of(tap * C2 + n * 16, 16), 16)
            hi_ref[at, :] = hi
            lo_ref[at, :] = lo
        return carry

    lax.fori_loop(0, C2 // 16, chunk, 0)

    def block(n, carry):
        at = pl.ds(pl.multiple_of(n * 256, 256), 256)
        both = mm(stacked_ref[...], hi_ref[:, at])
        low = mm(stacked_ref[0:C2, :], lo_ref[:, at])
        out_ref[:, at] = both[:C2] + both[C2:] + low
        return carry

    lax.fori_loop(0, 2, block, 0)


def coarse_halo(acc_ref, halo_ref, w_ref, edges, down=None):
    rows = halo_ref.shape[1]
    low_lane = iota((rows, 128), 1) < 64
    lane = iota((C2, 128), 1)
    a = (lane >> 3) & 7
    b = lane & 7
    sheets = []
    for pair in range(3):
        even = halo_ref[2 * pair]
        odd = halo_ref[2 * pair + 1]
        top = jnp.where(low_lane, even, pltpu.roll(odd, 64, 1))
        bottom = jnp.where(low_lane, pltpu.roll(even, 64, 1), odd)
        layer = jnp.concatenate([top, bottom], axis=0)
        if down is not None:
            layer = dot3(down, layer)
        his, los = [], []
        for tap in range(9):
            da, db = tap // 3 - 1, tap % 3 - 1
            keep = in_range(a + da, 8) & in_range(b + db, 8)
            moved = lane_roll(layer, -(8 * da + db))
            hi, lo = split(jnp.where(keep, moved, 0.0))
            his.append(hi)
            los.append(lo)
        eh, el = split(tap_columns(w_ref, face_taps(2 * pair), C2))
        oh, ol = split(tap_columns(w_ref, face_taps(2 * pair + 1), C2))
        both = mm(jnp.concatenate([eh, el, oh, ol], axis=0), jnp.concatenate(his, axis=0))
        low = mm(jnp.concatenate([eh, oh], axis=0), jnp.concatenate(los, axis=0))
        even_sum = both[0:C2] + both[C2 : 2 * C2] + low[0:C2]
        odd_sum = both[2 * C2 : 3 * C2] + both[3 * C2 :] + low[C2:]
        sheets.append(jnp.where(lane < 64, even_sum, odd_sum))
    return acc_ref[...] + dot2(jnp.concatenate(sheets, axis=1), edges)


def second_kernel(
    acc_ref,
    bias_ref,
    down_ref,
    arrived_ref,
    w_far,
    links_ref,
    slot_ref,
    second_ref,
    faces_ref,
    send_ref,
    spill_ref,
    halo_ref,
    w_near,
    sems,
    halo_sems,
    send_sems,
):
    arrive = fetch_halo([arrived_ref], [0, BRICKS], links_ref, halo_ref, halo_sems)
    (w_ref,) = late_copies([w_far], [w_near], sems)
    arrive()
    edges = coarse_edges()
    summed = coarse_halo(acc_ref, halo_ref, w_ref, edges, down_ref[...])
    second = silu(summed + bias_ref[...])
    second_ref[...] = second
    coarse_faces(second, edges, faces_ref)
    send_faces(faces_ref, slot_ref, [send_ref, spill_ref], send_sems)


def pool_rows(scale):
    row = iota((64, 512), 0)
    col = iota((64, 512), 1)
    target = (col >> 7) * 16 + ((col >> 4) & 3) * 4 + ((col >> 1) & 3)
    return jnp.where(target == row, scale, 0.0).astype(bf16)


def refined_kernel(
    acc_ref,
    second_ref,
    recv_ref,
    more_ref,
    relayed_ref,
    w_far,
    final_ref,
    refined_ref,
    coarse_ref,
    halo_ref,
    w_near,
    sems,
    halo_sems,
):
    arrive = fetch_halo([recv_ref, more_ref, relayed_ref], BOUNDS, final_ref, halo_ref, halo_sems)
    (w_ref,) = late_copies([w_far], [w_near], sems)
    arrive()
    summed = coarse_halo(acc_ref, halo_ref, w_ref, coarse_edges())
    refined = second_ref[...] + silu(summed)
    refined_ref[...] = refined
    pool = pool_rows(0.125)
    hi, lo = split(refined)
    coarse = mm(pool, hi, nt=True) + mm(pool, lo, nt=True)
    for member in range(MEMBERS):
        coarse_ref[member] = coarse


def attention_kernel(
    all_ref,
    down_far,
    wq_far,
    wk_far,
    wv_far,
    wo_far,
    up_far,
    refined_far,
    scale_ref,
    labels_ref,
    me_ref,
    slot_ref,
    joined_ref,
    faces_ref,
    send_ref,
    spill_ref,
    down_near,
    wq_near,
    wk_near,
    wv_near,
    wo_near,
    up_near,
    refined_near,
    sems,
    send_sems,
):
    down_ref, wq_ref, wk_ref, wv_ref, wo_ref, up_ref, refined_ref = late_copies(
        [down_far, wq_far, wk_far, wv_far, wo_far, up_far, refined_far],
        [down_near, wq_near, wk_near, wv_near, wo_near, up_near, refined_near],
        sems,
    )
    head_of = iota((C3, C3), 1) >> 6
    head_mean = jnp.where((iota((C3, C3), 0) >> 6) == head_of, 1.0 / HDIM, 0.0).astype(bf16)

    def normed(v):
        return v * lax.rsqrt(jnp.mean(v * v, axis=-1, keepdims=True) + EPSILON)

    def head_normed(v):
        return v * lax.rsqrt(dot2(v * v, head_mean) + EPSILON)

    tokens = dot3(all_ref[me_ref[1]], down_ref[...], nt=True)
    query = head_normed(dot3(normed(tokens), wq_ref[...]))
    gathered = all_ref[...].reshape(MEMBERS * TOKB, C2)
    everyone = normed(dot3(gathered, down_ref[...], nt=True))
    keys = head_normed(dot3(everyone, wk_ref[...]))
    values = dot3(everyone, wv_ref[...])
    lane_head = iota((TOKB, C3), 1) >> 6
    stacked = jnp.concatenate(
        [
            jnp.where(lane_head == h, query, 0.0) * (scale_ref[h] * (HDIM**-0.5))
            for h in range(HEADS)
        ],
        axis=0,
    )
    logits = dot3(stacked, keys, nt=True)
    brick_of = iota((1, MEMBERS * TOKB), 1) >> 6
    key_label = jnp.zeros((1, MEMBERS * TOKB), jnp.int32)
    for member in range(MEMBERS):
        key_label = jnp.where(brick_of == member, labels_ref[member], key_label)
    allowed = key_label == labels_ref[me_ref[1]]
    logits = jnp.where(allowed, logits, -1e30)
    peak = jnp.max(logits, axis=-1, keepdims=True)
    weight = jnp.where(allowed, jnp.exp(logits - peak), 0.0)
    total = jnp.sum(weight, axis=-1, keepdims=True)
    heads = dot3(weight, values) / total
    attended = jnp.zeros((TOKB, C3), f32)
    for h in range(HEADS):
        attended = jnp.where(lane_head == h, heads[h * TOKB : (h + 1) * TOKB], attended)
    mixed = tokens + dot3(attended, wo_ref[...])
    lifted = dot3(up_ref[...], mixed, nt=True)
    joined = refined_ref[...] + dot2(lifted, pool_rows(1.0))
    joined_ref[...] = joined
    coarse_faces(joined, coarse_edges(), faces_ref)
    send_faces(faces_ref, slot_ref, [send_ref, spill_ref], send_sems)


def decoded_kernel(
    acc_ref,
    recv_ref,
    more_ref,
    relayed_ref,
    w_far,
    up_far,
    first_far,
    final_ref,
    slot_ref,
    mix_ref,
    faces_ref,
    send_ref,
    spill_ref,
    halo_ref,
    w_near,
    up_near,
    first_near,
    sems,
    halo_sems,
    send_sems,
):
    arrive = fetch_halo([recv_ref, more_ref, relayed_ref], BOUNDS, final_ref, halo_ref, halo_sems)
    w_ref, up_ref, first_ref = late_copies(
        [w_far, up_far, first_far], [w_near, up_near, first_near], sems
    )
    arrive()
    decoded = silu(coarse_halo(acc_ref, halo_ref, w_ref, coarse_edges()))
    dropped = dot3(up_ref[...], decoded)
    row = iota((128, 1024), 0)
    col = iota((128, 1024), 1)
    source = (col >> 9) * 64 + ((col >> 5) & 7) * 8 + ((col >> 1) & 7)
    widen = as01(source == row)
    for quad in range(4):
        wide = dot2(dropped[:, quad * 128 : (quad + 1) * 128], widen)
        at = slice(quad * 1024, (quad + 1) * 1024)
        mix_ref[:, at] = silu(first_ref[:, at] + wide)
    fine_faces(mix_ref, faces_ref)
    send_faces(faces_ref, slot_ref, [send_ref, spill_ref], send_sems)


VMEM = pl.BlockSpec(memory_space=pltpu.VMEM)
SMEM = pl.BlockSpec(memory_space=pltpu.SMEM)
FAR = pl.BlockSpec(memory_space=pl.ANY)


def grant(mib):
    return pltpu.CompilerParams(vmem_limit_bytes=mib << 20)


def call(kernel, outs, args=(), scalars=(), scratch=(), pools=(), late=(), far=0, sends=0, mib=None):
    near = len(outs) - far
    copies = [pltpu.VMEM(v.shape, v.dtype) for v in late]
    sems = [pltpu.SemaphoreType.DMA((len(late),))] if late else []
    if pools:
        sems.append(pltpu.SemaphoreType.DMA((6,)))
    if sends:
        sems.append(pltpu.SemaphoreType.DMA((sends,)))
    return pl.pallas_call(
        kernel,
        out_shape=[jax.ShapeDtypeStruct(o, f32) for o in outs],
        in_specs=[VMEM] * len(args) + [FAR] * (len(pools) + len(late)) + [SMEM] * len(scalars),
        out_specs=[VMEM] * near + [FAR] * far,
        scratch_shapes=[*scratch, *copies, *sems],
        compiler_params=grant(mib) if mib else None,
    )(*args, *pools, *late, *scalars)


def route(rows, me):
    sizes = [6, GROUPS * SLOTS_G, 6, 1]
    return pl.pallas_call(
        route_kernel,
        out_shape=[jax.ShapeDtypeStruct((n,), jnp.int32) for n in sizes],
        in_specs=[VMEM, SMEM, SMEM],
        out_specs=[SMEM] * len(sizes),
        compiler_params=grant(4),
    )(rows, rows, me)


def table_kernel(links_ref, out_ref):
    lane = iota((BRICKS, 128), 1)
    row = jnp.full((BRICKS, 128), -1, jnp.int32)
    for face in range(6):
        row = jnp.where(lane == face, links_ref[face], row)
    out_ref[...] = row


def table_of(links):
    return pl.pallas_call(
        table_kernel,
        out_shape=jax.ShapeDtypeStruct((BRICKS, 128), jnp.int32),
        in_specs=[SMEM],
        out_specs=VMEM,
        compiler_params=grant(4),
    )(links)


def dense_halo(faces, links):
    owners = lax.broadcasted_iota(jnp.int32, (BRICKS, 6), 0)
    chosen = links[None, :] == owners
    parcel = jnp.zeros((BRICKS, *faces.shape[1:]), f32)
    for face in range(6):
        parcel = jnp.where(chosen[:, face, None, None], faces[face][None], parcel)
    arrived = lax.all_to_all(parcel, ALL, 0, 0, tiled=True)
    halos = []
    for face in range(6):
        layer = lax.dynamic_index_in_dim(
            arrived, jnp.maximum(links[face], 0), 0, keepdims=False
        )
        halos.append(jnp.where(links[face] >= 0, layer, 0.0))
    return jnp.stack(halos)


def along(axis, slots):
    count = lax.axis_size(axis)
    rows = slots.shape[0] // count * slots.shape[1]
    blocks = slots.reshape(count, rows, slots.shape[2])
    return lax.all_to_all(blocks, axis, 0, 0, tiled=True).reshape(slots.shape)


def exchange(faces, send, spill, relay, links, level):
    layer = faces.shape[1:]

    def nothing(operands):
        return jnp.zeros((MEMBERS, *layer), f32)

    def third(operands):
        return along("brick", operands[1])

    def dense(operands):
        halo = dense_halo(operands[0], links)
        return jnp.concatenate([halo, jnp.zeros((MEMBERS - 6, *layer), f32)])

    recv = along("brick", send)
    more = lax.switch(level, [nothing, third, dense], (faces, spill))
    (onward,) = call(
        relay_kernel,
        [(GROUPS * SLOTS_G, *layer)],
        [faces, recv, more],
        [relay],
        far=1,
        sends=GROUPS * SLOTS_G,
        mib=8,
    )
    return [recv, more, along("grp", onward)]


def per_device(
    noisy,
    neighbours,
    labels,
    conv_in,
    bias_in,
    down_fine,
    conv_mid,
    bias_mid,
    conv_res,
    conv_dec,
    down_mid,
    w_query,
    w_key,
    w_value,
    w_out,
    logit_scale,
    up_mid,
    up_fine,
    conv_out,
):
    links = neighbours[0]
    me = jnp.stack([lax.axis_index("grp"), lax.axis_index("brick")]).astype(jnp.int32)
    rows = lax.all_to_all(table_of(links), ALL, 0, 0, tiled=True)
    slot, relay, final, level = route(rows, me)
    level = level[0]

    def swap(faces, send, spill):
        return exchange(faces, send, spill, relay, links, level)

    fine_layer = (6, C1, 256)
    fine_sends = [(MEMBERS * SLOTS_B, C1, 256), (MEMBERS, C1, 256)]
    layer = (6, C2 // 2, 128)
    layer_sends = [(MEMBERS * SLOTS_B, C2 // 2, 128), (MEMBERS, C2 // 2, 128)]

    def fine_conv(v, w):
        return call(
            fine_conv_kernel,
            [(C1, S**3)],
            [v, w],
            scratch=[
                pltpu.VMEM((576, 4608), bf16),
                pltpu.VMEM((576, 4608), bf16),
                pltpu.VMEM((2 * C1, 27 * C1), bf16),
            ],
        )[0]

    def coarse_conv(v, w):
        return call(
            coarse_conv_kernel,
            [(C2, 512)],
            [v, w],
            scratch=[
                pltpu.VMEM((27 * C2, 512), bf16),
                pltpu.VMEM((27 * C2, 512), bf16),
                pltpu.VMEM((2 * C2, 27 * C2), bf16),
            ],
        )[0]

    fine_in = noisy[0]
    (faces,) = call(fine_face_kernel, [fine_layer], [fine_in])
    send, spill = call(
        pack_kernel, fine_sends, [faces], [slot], far=2, sends=6, mib=8
    )
    acc = fine_conv(fine_in, conv_in)
    pools = swap(faces, send, spill)
    mid, first, send = call(
        fine_first_kernel,
        [(C2, 512), (C1, S**3), (BRICKS, C1 // 2, 128)],
        [bias_in[:, None], down_fine],
        [final, links],
        [
            pltpu.VMEM(fine_layer, f32),
            pltpu.VMEM((C1, S**3), f32),
            pltpu.VMEM((6, C1 // 2, 128), f32),
        ],
        pools,
        [acc, conv_in],
        far=2,
        sends=6,
    )
    acc = coarse_conv(mid, conv_mid)
    arrived = lax.all_to_all(send, ALL, 0, 0, tiled=True)
    second, faces, send, spill = call(
        second_kernel,
        [(C2, 512), layer, *layer_sends],
        [acc, bias_mid[:, None], down_fine],
        [links, slot],
        [pltpu.VMEM((6, C1 // 2, 128), f32)],
        [arrived],
        [conv_mid],
        far=2,
        sends=6,
    )
    acc = coarse_conv(second, conv_res)
    pools = swap(faces, send, spill)
    refined, coarse = call(
        refined_kernel,
        [(C2, 512), (MEMBERS, TOKB, C2)],
        [acc, second],
        [final],
        [pltpu.VMEM(layer, f32)],
        pools,
        [conv_res],
    )
    everyone = along("brick", coarse)
    joined, faces, send, spill = call(
        attention_kernel,
        [(C2, 512), layer, *layer_sends],
        [everyone],
        [logit_scale, labels[0], me, slot],
        late=[down_mid, w_query, w_key, w_value, w_out, up_mid, refined],
        far=2,
        sends=6,
    )
    acc = coarse_conv(joined, conv_dec)
    pools = swap(faces, send, spill)
    mix, faces, send, spill = call(
        decoded_kernel,
        [(C1, S**3), fine_layer, *fine_sends],
        [acc],
        [final, slot],
        [pltpu.VMEM(layer, f32)],
        pools,
        [conv_dec, up_fine, first],
        far=2,
        sends=6,
    )
    acc = fine_conv(mix, conv_out)
    pools = swap(faces, send, spill)
    (result,) = call(
        fine_last_kernel,
        [(C1, S**3)],
        [],
        [final],
        [pltpu.VMEM(fine_layer, f32)],
        pools,
        [acc, conv_out],
    )
    return result[None]


def solution(mesh):
    in_specs = (
        P(("grp", "brick"), None, None),
        P(("grp", "brick"), None),
        P("grp", None),
    ) + (P(),) * 16
    out_specs = P(("grp", "brick"), None, None)
    return jax.shard_map(
        per_device, mesh=mesh, in_specs=in_specs, out_specs=out_specs, check_vma=False
    )
```

```python
import jax
import jax.numpy as jnp
from jax import lax
from jax.experimental import pallas as pl
from jax.experimental.pallas import tpu as pltpu
from jax.sharding import PartitionSpec as P

S = 16
C1 = 64
C2 = 128
C3 = 256
HEADS = 4
HDIM = 64
TOKB = 64
BRICKS = 128
GROUPS = 8
MEMBERS = 16
SLOTS_B = 2
SLOTS_G = 3
FROM_B = 6
FROM_X = FROM_B + MEMBERS * SLOTS_B
FROM_G = FROM_X + MEMBERS
FROM_END = FROM_G + GROUPS * SLOTS_G
EPSILON = 1e-06
ALL = ("grp", "brick")

f32 = jnp.float32
bf16 = jnp.bfloat16


def split(v):
    hi = v.astype(bf16)
    return hi, (v - hi.astype(f32)).astype(bf16)


def mm(a, b, nt=False):
    return lax.dot_general(
        a, b, (((1,), (1 if nt else 0,)), ((), ())), preferred_element_type=f32
    )


def dot3(a, b, nt=False):
    rows = a.shape[0]
    ah, al = split(a)
    bh, bl = split(b)
    both = mm(jnp.concatenate([ah, al], axis=0), bh, nt)
    return both[:rows] + both[rows:] + mm(ah, bl, nt)


def dot2(a, selector, nt=False):
    rows = a.shape[0]
    ah, al = split(a)
    both = mm(jnp.concatenate([ah, al], axis=0), selector, nt)
    return both[:rows] + both[rows:]


def iota(shape, dim):
    return lax.broadcasted_iota(jnp.int32, shape, dim)


def as01(mask):
    return jnp.where(mask, 1.0, 0.0).astype(bf16)


def silu(v):
    return v / (1.0 + jnp.exp(-v))


def lane_roll(v, shift):
    amount = shift % v.shape[1]
    return v if amount == 0 else pltpu.roll(v, amount, 1)


def in_range(index, edge):
    return (index >= 0) & (index < edge)


def face_taps(face):
    side = 2 * (face % 2)
    if face < 2:
        return [9 * side + 3 * a + b for a in range(3) for b in range(3)]
    if face < 4:
        return [9 * a + 3 * side + b for a in range(3) for b in range(3)]
    return [9 * a + 3 * b + side for a in range(3) for b in range(3)]


def tap_columns(w_ref, taps, channels):
    runs = []
    for t in taps:
        if runs and runs[-1][1] == t:
            runs[-1][1] = t + 1
        else:
            runs.append([t, t + 1])
    pieces = [w_ref[:, lo * channels : hi * channels] for lo, hi in runs]
    return pieces[0] if len(pieces) == 1 else jnp.concatenate(pieces, axis=1)


def coarse_edges():
    row = iota((384, 512), 0)
    col = iota((384, 512), 1)
    pair = row >> 7
    edge = ((row >> 6) & 1) * 7
    a = (row >> 3) & 7
    b = row & 7
    x = col >> 6
    y = (col >> 3) & 7
    z = col & 7
    along = jnp.where(pair == 0, x, jnp.where(pair == 1, y, z))
    first = jnp.where(pair == 0, y, x)
    last = jnp.where(pair == 2, y, z)
    return as01((along == edge) & (first == a) & (last == b))


def fine_sides():
    row = iota((256, 256), 0)
    col = iota((256, 256), 1)
    edge = (row >> 7) * 15
    return as01(((col & 15) == edge) & ((col >> 4) == (row & 15)))


def fine_sides_t():
    row = iota((256, 256), 0)
    col = iota((256, 256), 1)
    edge = (col >> 7) * 15
    return as01(((row & 15) == edge) & ((row >> 4) == (col & 15)))


class Late:
    def __init__(self, far_ref, near_ref, sem):
        self.near_ref = near_ref
        self.copy = pltpu.make_async_copy(far_ref, near_ref, sem)
        self.copy.start()
        self.here = False

    def __getitem__(self, index):
        if not self.here:
            self.copy.wait()
            self.here = True
        return self.near_ref[index]


def late_copies(far_refs, near_refs, sems):
    return [
        Late(far, near, sems.at[n]) for n, (far, near) in enumerate(zip(far_refs, near_refs))
    ]


def send_faces(faces_ref, slot_ref, send_refs, sems):
    def each(act):
        for face in range(6):
            slot = slot_ref[face]
            base = 0
            for send_ref in send_refs:
                count = send_ref.shape[0]
                inside = (slot >= base) & (slot < base + count)

                @pl.when(inside)
                def _():
                    act(
                        pltpu.make_async_copy(
                            faces_ref.at[face], send_ref.at[slot - base], sems.at[face]
                        )
                    )

                base += count

    each(lambda copy: copy.start())
    each(lambda copy: copy.wait())


def fetch_halo(pools, bounds, index_ref, halo_ref, sems):
    def each(act):
        for face in range(6):
            source = index_ref[face]
            for pool, low, high in zip(pools, bounds[:-1], bounds[1:]):

                @pl.when((source >= low) & (source < high))
                def _():
                    act(
                        pltpu.make_async_copy(
                            pool.at[source - low], halo_ref.at[face], sems.at[face]
                        )
                    )

    each(lambda copy: copy.start())
    for face in range(6):

        @pl.when(index_ref[face] < 0)
        def _():
            halo_ref[face] = jnp.zeros(halo_ref.shape[1:], f32)

    return lambda: each(lambda copy: copy.wait())


BOUNDS = [FROM_B, FROM_X, FROM_G, FROM_END]


def coarse_faces(v, edges, faces_ref):
    rows = v.shape[0] // 2
    picked = dot2(v, edges, nt=True)
    low = iota((rows, 128), 1) < 64
    for pair in range(3):
        block = picked[:, pair * 128 : (pair + 1) * 128]
        top = block[:rows]
        bottom = block[rows:]
        faces_ref[2 * pair] = jnp.where(low, top, pltpu.roll(bottom, 64, 1))
        faces_ref[2 * pair + 1] = jnp.where(low, pltpu.roll(top, 64, 1), bottom)


def fine_faces(v_ref, faces_ref):
    faces_ref[0] = v_ref[:, 0:256]
    faces_ref[1] = v_ref[:, 3840:4096]
    sides = fine_sides_t()
    at_x = iota((C1, 128), 1) >> 4
    for half in range(2):
        found = [None] * 4
        for k in range(8):
            start = (half * 8 + k) * 256
            part = v_ref[:, start : start + 256]
            near = dot2(part, sides)
            new = [
                lane_roll(part[:, :128], 16 * k),
                lane_roll(part[:, 128:], 16 * k - 112),
                near[:, :128],
                near[:, 128:],
            ]
            if k == 0:
                found = new
            else:
                found = [jnp.where(at_x == k, n, o) for n, o in zip(new, found)]
        for kind in range(4):
            faces_ref[2 + kind, :, half * 128 : (half + 1) * 128] = found[kind]


def route_kernel(all_ref, table_ref, me_ref, slot_ref, relay_ref, final_ref, level_ref):
    g = me_ref[0]
    b = me_ref[1]
    me = g * MEMBERS + b
    here = all_ref[...]
    brick = iota((BRICKS, 128), 0)
    same_b = jnp.zeros((BRICKS, 128), f32)
    same_g = jnp.zeros((BRICKS, 128), f32)
    for back in range(1, 6):
        there = pltpu.roll(here, back, 1)
        known = there >= 0
        same_b += jnp.where(known & ((there & 15) == (here & 15)), 1.0, 0.0)
        same_g += jnp.where(known & ((there >> 4) == (here >> 4)), 1.0, 0.0)
    same_b = jnp.where((here >= 0) & ((here & 15) != (brick & 15)), same_b, 0.0)
    same_g = jnp.where((here >= 0) & ((here >> 4) != (brick >> 4)), same_g, 0.0)
    most_b = jnp.max(same_b).astype(jnp.int32)
    most_g = jnp.max(same_g).astype(jnp.int32)
    crowded = (most_b > SLOTS_B) | (most_g >= SLOTS_G)
    level = jnp.where(crowded, 2, jnp.where(most_b == SLOTS_B, 1, 0))
    level_ref[0] = level

    def rank_b(i, face, member):
        count = jnp.int32(0)
        for other in range(5):
            j = table_ref[i, other]
            hit = (j >= 0) & ((j & 15) == member) & (other < face)
            count = count + jnp.where(hit, 1, 0)
        return count

    def rank_g(j, face, group):
        count = jnp.int32(0)
        for other in range(face):
            i = table_ref[j, other]
            hit = (i >= 0) & ((i >> 4) == group)
            count = count + jnp.where(hit, 1, 0)
        return count

    def slot_b(member, rank):
        low = member * SLOTS_B + jnp.minimum(rank, SLOTS_B - 1)
        return jnp.where(rank < SLOTS_B, low, MEMBERS * SLOTS_B + member)

    for face in range(6):
        j = table_ref[me, face]
        member = j & 15
        rank = rank_b(me, face, member)
        fine = (j >= 0) & (member != b) & (rank <= SLOTS_B)
        slot_ref[face] = jnp.where(fine, slot_b(member, rank), -1)
    for slot in range(GROUPS * SLOTS_G):
        relay_ref[slot] = jnp.int32(-1)

    def relay_to(group, carry):
        j = group * MEMBERS + b
        for face in range(6):
            i = table_ref[j, face]
            mine = (i >= 0) & ((i >> 4) == g) & (group != g)
            safe = jnp.maximum(i, 0)
            rank = rank_g(j, face, g)
            first = rank_b(safe, face ^ 1, b)
            member = safe & 15
            source = jnp.where(member == b, face ^ 1, FROM_B + slot_b(member, first))
            fits = mine & (rank < SLOTS_G) & ((member == b) | (first <= SLOTS_B))

            @pl.when(fits)
            def _():
                relay_ref[group * SLOTS_G + rank] = source

        return carry

    lax.fori_loop(0, GROUPS, relay_to, 0)
    for face in range(6):
        i = table_ref[me, face]
        safe = jnp.maximum(i, 0)
        first = rank_b(safe, face ^ 1, b)
        group = safe >> 4
        rank = jnp.minimum(rank_g(me, face, group), SLOTS_G - 1)
        source = jnp.where(
            group == g,
            FROM_B + slot_b(safe & 15, first),
            FROM_G + group * SLOTS_G + rank,
        )
        source = jnp.where(level == 2, FROM_X + face, source)
        final_ref[face] = jnp.where(i >= 0, source, -1)


def relay_kernel(faces_ref, recv_ref, more_ref, index_ref, out_ref, sems):
    def each(act):
        def one(slot, carry):
            source = index_ref[slot]
            starts = [0, FROM_B, FROM_X, FROM_G]
            for pool, low, high in zip(
                (faces_ref, recv_ref, more_ref), starts[:-1], starts[1:]
            ):

                @pl.when((source >= low) & (source < high))
                def _():
                    act(
                        pltpu.make_async_copy(
                            pool.at[source - low], out_ref.at[slot], sems.at[slot]
                        )
                    )

            return carry

        lax.fori_loop(0, GROUPS * SLOTS_G, one, 0)

    each(lambda copy: copy.start())
    each(lambda copy: copy.wait())


def fine_face_kernel(v_ref, faces_ref):
    fine_faces(v_ref, faces_ref)


def pack_kernel(faces_ref, slot_ref, send_ref, spill_ref, sems):
    send_faces(faces_ref, slot_ref, [send_ref, spill_ref], sems)


def split_weights(w_ref, stacked_ref):
    rows = w_ref.shape[0]
    hi, lo = split(w_ref[...])
    stacked_ref[0:rows, :] = hi
    stacked_ref[rows : 2 * rows, :] = lo


def fine_conv_kernel(v_ref, w_ref, out_ref, hi_ref, lo_ref, stacked_ref):
    split_weights(w_ref, stacked_ref)
    for ref in (hi_ref, lo_ref):
        ref[:, 0:256] = jnp.zeros((576, 256), bf16)
        ref[:, 4352:4608] = jnp.zeros((576, 256), bf16)
    lane = iota((C1, 256), 1)
    y = lane >> 4
    z = lane & 15

    def plane(x, carry):
        part = v_ref[:, pl.ds(pl.multiple_of(x * 256, 256), 256)]
        for tap in range(9):
            dy, dz = tap // 3 - 1, tap % 3 - 1
            moved = lane_roll(part, -(16 * dy + dz))
            keep = in_range(y + dy, S) & in_range(z + dz, S)
            hi, lo = split(jnp.where(keep, moved, 0.0))
            at = pl.ds(pl.multiple_of(x * 256 + 256, 256), 256)
            hi_ref[tap * C1 : (tap + 1) * C1, at] = hi
            lo_ref[tap * C1 : (tap + 1) * C1, at] = lo
        return carry

    lax.fori_loop(0, S, plane, 0)

    def block(n, carry):
        def gathered(ref):
            return jnp.concatenate(
                [
                    ref[:, pl.ds(pl.multiple_of(n * 256 + dx * 256, 256), 256)]
                    for dx in range(3)
                ],
                axis=0,
            )

        both = mm(stacked_ref[...], gathered(hi_ref))
        low = mm(stacked_ref[0:C1, :], gathered(lo_ref))
        at = pl.ds(pl.multiple_of(n * 256, 256), 256)
        out_ref[:, at] = both[:C1] + both[C1:] + low
        return carry

    lax.fori_loop(0, S, block, 0)


def fine_halo(acc_ref, halo_ref, w_ref, out_ref):
    lane = iota((C1, 256), 1)
    a = lane >> 4
    b = lane & 15
    sheets = []
    for face in range(6):
        layer = halo_ref[face]
        his, los = [], []
        for tap in range(9):
            da, db = tap // 3 - 1, tap % 3 - 1
            keep = in_range(a + da, S) & in_range(b + db, S)
            moved = lane_roll(layer, -(16 * da + db))
            hi, lo = split(jnp.where(keep, moved, 0.0))
            his.append(hi)
            los.append(lo)
        wh, wl = split(tap_columns(w_ref, face_taps(face), C1))
        both = mm(jnp.concatenate([wh, wl], axis=0), jnp.concatenate(his, axis=0))
        low = mm(wh, jnp.concatenate(los, axis=0))
        sheets.append(both[:C1] + both[C1:] + low)
    sides = fine_sides()
    at_x = (iota((2 * C1, 256), 1) >> 4) & 7
    lane = iota((C1, 128), 1)
    for half in range(2):
        at = slice(half * 128, (half + 1) * 128)
        near = jnp.concatenate([sheets[4][:, at], sheets[5][:, at]], axis=1)
        hi, lo = split(near)
        spread = jnp.concatenate([hi, lo], axis=0)
        for k in range(8):
            x = half * 8 + k
            both = mm(spread * as01(at_x == k), sides)
            start = x * 256
            total = acc_ref[:, start : start + 256] + both[:C1] + both[C1:]
            low = lane_roll(sheets[2][:, at], -16 * k)
            high = lane_roll(sheets[3][:, at], 112 - 16 * k)
            ends = jnp.concatenate(
                [jnp.where(lane < 16, low, 0.0), jnp.where(lane >= 112, high, 0.0)], axis=1
            )
            total = total + ends
            if x == 0:
                total = total + sheets[0]
            if x == S - 1:
                total = total + sheets[1]
            out_ref[:, start : start + 256] = total


def fine_last_kernel(
    recv_ref,
    more_ref,
    relayed_ref,
    acc_far,
    w_far,
    final_ref,
    out_ref,
    halo_ref,
    acc_near,
    w_near,
    sems,
    halo_sems,
):
    arrive = fetch_halo([recv_ref, more_ref, relayed_ref], BOUNDS, final_ref, halo_ref, halo_sems)
    acc_ref, w_ref = late_copies([acc_far, w_far], [acc_near, w_near], sems)
    arrive()
    fine_halo(acc_ref, halo_ref, w_ref, out_ref)


def fine_first_kernel(
    bias_ref,
    down_ref,
    recv_ref,
    more_ref,
    relayed_ref,
    acc_far,
    w_far,
    final_ref,
    links_ref,
    mid_ref,
    first_far,
    send_ref,
    halo_ref,
    first_ref,
    faces_ref,
    acc_near,
    w_near,
    sems,
    halo_sems,
    send_sems,
):
    arrive = fetch_halo([recv_ref, more_ref, relayed_ref], BOUNDS, final_ref, halo_ref, halo_sems)
    acc_ref, w_ref = late_copies([acc_far, w_far], [acc_near, w_near], sems)
    arrive()
    fine_halo(acc_ref, halo_ref, w_ref, first_ref)
    first_ref[...] = silu(first_ref[...] + bias_ref[...])
    keep = pltpu.make_async_copy(first_ref, first_far, sems.at[0])
    keep.start()
    row = iota((512, 128), 0)
    col = iota((512, 128), 1)
    target = (row >> 8) * 64 + ((row >> 5) & 7) * 8 + ((row >> 1) & 7)
    pool = jnp.where(target == col, 0.125, 0.0).astype(bf16)
    parts = []
    for quad in range(4):
        planes = [
            first_ref[:, (4 * quad + k) * 256 : (4 * quad + k + 1) * 256] for k in range(4)
        ]
        pair = jnp.concatenate([planes[0] + planes[1], planes[2] + planes[3]], axis=1)
        parts.append(dot2(pair, pool))
    shrunk = jnp.concatenate(parts, axis=1)
    mid_ref[...] = dot3(down_ref[...], shrunk)
    coarse_faces(shrunk, coarse_edges(), faces_ref)
    send_faces(faces_ref, links_ref, [send_ref], send_sems)
    keep.wait()


def coarse_conv_kernel(v_ref, w_ref, out_ref, hi_ref, lo_ref, stacked_ref):
    split_weights(w_ref, stacked_ref)
    lane = iota((16, 512), 1)
    x = lane >> 6
    y = (lane >> 3) & 7
    z = lane & 7

    def chunk(n, carry):
        part = v_ref[pl.ds(pl.multiple_of(n * 16, 16), 16), :]
        for tap in range(27):
            dx, dy, dz = tap // 9 - 1, tap // 3 % 3 - 1, tap % 3 - 1
            keep = in_range(x + dx, 8) & in_range(y + dy, 8) & in_range(z + dz, 8)
            moved = lane_roll(part, -(64 * dx + 8 * dy + dz))
            hi, lo = split(jnp.where(keep, moved, 0.0))
            at = pl.ds(pl.multiple_of(tap * C2 + n * 16, 16), 16)
            hi_ref[at, :] = hi
            lo_ref[at, :] = lo
        return carry

    lax.fori_loop(0, C2 // 16, chunk, 0)

    out_ref[...] = jnp.zeros((C2, 512), f32)

    def block(triple, carry):
        at = pl.ds(pl.multiple_of(triple * 3 * C2, 128), 3 * C2)
        both = mm(stacked_ref[:, at], hi_ref[at, :])
        low = mm(stacked_ref[0:C2, at], lo_ref[at, :])
        out_ref[...] += both[:C2] + both[C2:] + low
        return carry

    lax.fori_loop(0, 9, block, 0)


def coarse_halo(acc_ref, halo_ref, w_ref, edges, down=None):
    rows = halo_ref.shape[1]
    low_lane = iota((rows, 128), 1) < 64
    lane = iota((C2, 128), 1)
    a = (lane >> 3) & 7
    b = lane & 7
    sheets = []
    for pair in range(3):
        even = halo_ref[2 * pair]
        odd = halo_ref[2 * pair + 1]
        top = jnp.where(low_lane, even, pltpu.roll(odd, 64, 1))
        bottom = jnp.where(low_lane, pltpu.roll(even, 64, 1), odd)
        layer = jnp.concatenate([top, bottom], axis=0)
        if down is not None:
            layer = dot3(down, layer)
        his, los = [], []
        for tap in range(9):
            da, db = tap // 3 - 1, tap % 3 - 1
            keep = in_range(a + da, 8) & in_range(b + db, 8)
            moved = lane_roll(layer, -(8 * da + db))
            hi, lo = split(jnp.where(keep, moved, 0.0))
            his.append(hi)
            los.append(lo)
        eh, el = split(tap_columns(w_ref, face_taps(2 * pair), C2))
        oh, ol = split(tap_columns(w_ref, face_taps(2 * pair + 1), C2))
        both = mm(jnp.concatenate([eh, el, oh, ol], axis=0), jnp.concatenate(his, axis=0))
        low = mm(jnp.concatenate([eh, oh], axis=0), jnp.concatenate(los, axis=0))
        even_sum = both[0:C2] + both[C2 : 2 * C2] + low[0:C2]
        odd_sum = both[2 * C2 : 3 * C2] + both[3 * C2 :] + low[C2:]
        sheets.append(jnp.where(lane < 64, even_sum, odd_sum))
    return acc_ref[...] + dot2(jnp.concatenate(sheets, axis=1), edges)


def second_kernel(
    acc_ref,
    bias_ref,
    down_ref,
    arrived_ref,
    w_far,
    links_ref,
    slot_ref,
    second_ref,
    faces_ref,
    send_ref,
    spill_ref,
    halo_ref,
    w_near,
    sems,
    halo_sems,
    send_sems,
):
    arrive = fetch_halo([arrived_ref], [0, BRICKS], links_ref, halo_ref, halo_sems)
    (w_ref,) = late_copies([w_far], [w_near], sems)
    arrive()
    edges = coarse_edges()
    summed = coarse_halo(acc_ref, halo_ref, w_ref, edges, down_ref[...])
    second = silu(summed + bias_ref[...])
    second_ref[...] = second
    coarse_faces(second, edges, faces_ref)
    send_faces(faces_ref, slot_ref, [send_ref, spill_ref], send_sems)


def pool_rows(scale):
    row = iota((64, 512), 0)
    col = iota((64, 512), 1)
    target = (col >> 7) * 16 + ((col >> 4) & 3) * 4 + ((col >> 1) & 3)
    return jnp.where(target == row, scale, 0.0).astype(bf16)


def refined_kernel(
    acc_ref,
    second_ref,
    recv_ref,
    more_ref,
    relayed_ref,
    w_far,
    final_ref,
    refined_ref,
    coarse_ref,
    halo_ref,
    w_near,
    sems,
    halo_sems,
):
    arrive = fetch_halo([recv_ref, more_ref, relayed_ref], BOUNDS, final_ref, halo_ref, halo_sems)
    (w_ref,) = late_copies([w_far], [w_near], sems)
    arrive()
    summed = coarse_halo(acc_ref, halo_ref, w_ref, coarse_edges())
    refined = second_ref[...] + silu(summed)
    refined_ref[...] = refined
    pool = pool_rows(0.125)
    hi, lo = split(refined)
    coarse = mm(pool, hi, nt=True) + mm(pool, lo, nt=True)
    for member in range(MEMBERS):
        coarse_ref[member] = coarse


def attention_kernel(
    all_ref,
    refined_ref,
    down_ref,
    wq_ref,
    wk_ref,
    wv_ref,
    wo_ref,
    up_ref,
    scale_ref,
    labels_ref,
    me_ref,
    slot_ref,
    joined_ref,
    faces_ref,
    send_ref,
    spill_ref,
    send_sems,
):
    head_of = iota((C3, C3), 1) >> 6
    head_mean = jnp.where((iota((C3, C3), 0) >> 6) == head_of, 1.0 / HDIM, 0.0).astype(bf16)

    def normed(v):
        return v * lax.rsqrt(jnp.mean(v * v, axis=-1, keepdims=True) + EPSILON)

    def head_normed(v):
        return v * lax.rsqrt(dot2(v * v, head_mean) + EPSILON)

    tokens = dot3(all_ref[me_ref[1]], down_ref[...], nt=True)
    query = head_normed(dot3(normed(tokens), wq_ref[...]))
    gathered = all_ref[...].reshape(MEMBERS * TOKB, C2)
    everyone = normed(dot3(gathered, down_ref[...], nt=True))
    keys = head_normed(dot3(everyone, wk_ref[...]))
    values = dot3(everyone, wv_ref[...])
    lane_head = iota((TOKB, C3), 1) >> 6
    stacked = jnp.concatenate(
        [
            jnp.where(lane_head == h, query, 0.0) * (scale_ref[h] * (HDIM**-0.5))
            for h in range(HEADS)
        ],
        axis=0,
    )
    logits = dot3(stacked, keys, nt=True)
    brick_of = iota((1, MEMBERS * TOKB), 1) >> 6
    key_label = jnp.zeros((1, MEMBERS * TOKB), jnp.int32)
    for member in range(MEMBERS):
        key_label = jnp.where(brick_of == member, labels_ref[member], key_label)
    allowed = key_label == labels_ref[me_ref[1]]
    logits = jnp.where(allowed, logits, -1e30)
    peak = jnp.max(logits, axis=-1, keepdims=True)
    weight = jnp.where(allowed, jnp.exp(logits - peak), 0.0)
    total = jnp.sum(weight, axis=-1, keepdims=True)
    heads = dot3(weight, values) / total
    attended = jnp.zeros((TOKB, C3), f32)
    for h in range(HEADS):
        attended = jnp.where(lane_head == h, heads[h * TOKB : (h + 1) * TOKB], attended)
    mixed = tokens + dot3(attended, wo_ref[...])
    lifted = dot3(up_ref[...], mixed, nt=True)
    joined = refined_ref[...] + dot2(lifted, pool_rows(1.0))
    joined_ref[...] = joined
    coarse_faces(joined, coarse_edges(), faces_ref)
    send_faces(faces_ref, slot_ref, [send_ref, spill_ref], send_sems)


def decoded_kernel(
    acc_ref,
    recv_ref,
    more_ref,
    relayed_ref,
    w_far,
    up_far,
    first_far,
    final_ref,
    slot_ref,
    mix_ref,
    faces_ref,
    send_ref,
    spill_ref,
    halo_ref,
    w_near,
    up_near,
    first_near,
    sems,
    halo_sems,
    send_sems,
):
    arrive = fetch_halo([recv_ref, more_ref, relayed_ref], BOUNDS, final_ref, halo_ref, halo_sems)
    w_ref, up_ref, first_ref = late_copies(
        [w_far, up_far, first_far], [w_near, up_near, first_near], sems
    )
    arrive()
    decoded = silu(coarse_halo(acc_ref, halo_ref, w_ref, coarse_edges()))
    dropped = dot3(up_ref[...], decoded)
    row = iota((128, 1024), 0)
    col = iota((128, 1024), 1)
    source = (col >> 9) * 64 + ((col >> 5) & 7) * 8 + ((col >> 1) & 7)
    widen = as01(source == row)
    for quad in range(4):
        wide = dot2(dropped[:, quad * 128 : (quad + 1) * 128], widen)
        at = slice(quad * 1024, (quad + 1) * 1024)
        mix_ref[:, at] = silu(first_ref[:, at] + wide)
    fine_faces(mix_ref, faces_ref)
    send_faces(faces_ref, slot_ref, [send_ref, spill_ref], send_sems)


VMEM = pl.BlockSpec(memory_space=pltpu.VMEM)
SMEM = pl.BlockSpec(memory_space=pltpu.SMEM)
FAR = pl.BlockSpec(memory_space=pl.ANY)


def grant(mib):
    return pltpu.CompilerParams(vmem_limit_bytes=mib << 20)


def call(kernel, outs, args=(), scalars=(), scratch=(), pools=(), late=(), far=0, sends=0, mib=None):
    near = len(outs) - far
    copies = [pltpu.VMEM(v.shape, v.dtype) for v in late]
    sems = [pltpu.SemaphoreType.DMA((len(late),))] if late else []
    if pools:
        sems.append(pltpu.SemaphoreType.DMA((6,)))
    if sends:
        sems.append(pltpu.SemaphoreType.DMA((sends,)))
    return pl.pallas_call(
        kernel,
        out_shape=[jax.ShapeDtypeStruct(o, f32) for o in outs],
        in_specs=[VMEM] * len(args) + [FAR] * (len(pools) + len(late)) + [SMEM] * len(scalars),
        out_specs=[VMEM] * near + [FAR] * far,
        scratch_shapes=[*scratch, *copies, *sems],
        compiler_params=grant(mib) if mib else None,
    )(*args, *pools, *late, *scalars)


def route(rows, me):
    sizes = [6, GROUPS * SLOTS_G, 6, 1]
    return pl.pallas_call(
        route_kernel,
        out_shape=[jax.ShapeDtypeStruct((n,), jnp.int32) for n in sizes],
        in_specs=[VMEM, SMEM, SMEM],
        out_specs=[SMEM] * len(sizes),
        compiler_params=grant(4),
    )(rows, rows, me)


def table_kernel(links_ref, out_ref):
    lane = iota((BRICKS, 128), 1)
    row = jnp.full((BRICKS, 128), -1, jnp.int32)
    for face in range(6):
        row = jnp.where(lane == face, links_ref[face], row)
    out_ref[...] = row


def table_of(links):
    return pl.pallas_call(
        table_kernel,
        out_shape=jax.ShapeDtypeStruct((BRICKS, 128), jnp.int32),
        in_specs=[SMEM],
        out_specs=VMEM,
        compiler_params=grant(4),
    )(links)


def ring_halo(faces, links):
    me = lax.axis_index(ALL)
    ring = [(i, (i + 1) % BRICKS) for i in range(BRICKS)]

    def one(step, held):
        passing, halo = held
        passing = lax.ppermute(passing, ALL, ring)
        source = (me - step) % BRICKS
        wanted = [
            jnp.where(links[face] == source, passing[face ^ 1], halo[face])
            for face in range(6)
        ]
        return passing, jnp.stack(wanted)

    return lax.fori_loop(1, BRICKS, one, (faces, jnp.zeros_like(faces)))[1]


def along(axis, slots):
    count = lax.axis_size(axis)
    rows = slots.shape[0] // count * slots.shape[1]
    blocks = slots.reshape(count, rows, slots.shape[2])
    return lax.all_to_all(blocks, axis, 0, 0, tiled=True).reshape(slots.shape)


def exchange(faces, send, spill, relay, links, level):
    layer = faces.shape[1:]

    def nothing(operands):
        return jnp.zeros((MEMBERS, *layer), f32)

    def third(operands):
        return along("brick", operands[1])

    def ring(operands):
        halo = ring_halo(operands[0], links)
        return jnp.concatenate([halo, jnp.zeros((MEMBERS - 6, *layer), f32)])

    recv = along("brick", send)
    more = lax.switch(level, [nothing, third, ring], (faces, spill))
    (onward,) = call(
        relay_kernel,
        [(GROUPS * SLOTS_G, *layer)],
        [faces, recv, more],
        [relay],
        far=1,
        sends=GROUPS * SLOTS_G,
        mib=8,
    )
    return [recv, more, along("grp", onward)]


def per_device(
    noisy,
    neighbours,
    labels,
    conv_in,
    bias_in,
    down_fine,
    conv_mid,
    bias_mid,
    conv_res,
    conv_dec,
    down_mid,
    w_query,
    w_key,
    w_value,
    w_out,
    logit_scale,
    up_mid,
    up_fine,
    conv_out,
):
    links = neighbours[0]
    me = jnp.stack([lax.axis_index("grp"), lax.axis_index("brick")]).astype(jnp.int32)
    rows = lax.all_to_all(table_of(links), ALL, 0, 0, tiled=True)
    slot, relay, final, level = route(rows, me)
    level = level[0]

    def swap(faces, send, spill):
        return exchange(faces, send, spill, relay, links, level)

    fine_layer = (6, C1, 256)
    fine_sends = [(MEMBERS * SLOTS_B, C1, 256), (MEMBERS, C1, 256)]
    layer = (6, C2 // 2, 128)
    layer_sends = [(MEMBERS * SLOTS_B, C2 // 2, 128), (MEMBERS, C2 // 2, 128)]

    def fine_conv(v, w):
        return call(
            fine_conv_kernel,
            [(C1, S**3)],
            [v, w],
            scratch=[
                pltpu.VMEM((576, 4608), bf16),
                pltpu.VMEM((576, 4608), bf16),
                pltpu.VMEM((2 * C1, 27 * C1), bf16),
            ],
        )[0]

    def coarse_conv(v, w):
        return call(
            coarse_conv_kernel,
            [(C2, 512)],
            [v, w],
            scratch=[
                pltpu.VMEM((27 * C2, 512), bf16),
                pltpu.VMEM((27 * C2, 512), bf16),
                pltpu.VMEM((2 * C2, 27 * C2), bf16),
            ],
        )[0]

    fine_in = noisy[0]
    (faces,) = call(fine_face_kernel, [fine_layer], [fine_in])
    send, spill = call(
        pack_kernel, fine_sends, [faces], [slot], far=2, sends=6, mib=8
    )
    acc = fine_conv(fine_in, conv_in)
    pools = swap(faces, send, spill)
    mid, first, send = call(
        fine_first_kernel,
        [(C2, 512), (C1, S**3), (BRICKS, C1 // 2, 128)],
        [bias_in[:, None], down_fine],
        [final, links],
        [
            pltpu.VMEM(fine_layer, f32),
            pltpu.VMEM((C1, S**3), f32),
            pltpu.VMEM((6, C1 // 2, 128), f32),
        ],
        pools,
        [acc, conv_in],
        far=2,
        sends=6,
    )
    acc = coarse_conv(mid, conv_mid)
    arrived = lax.all_to_all(send, ALL, 0, 0, tiled=True)
    second, faces, send, spill = call(
        second_kernel,
        [(C2, 512), layer, *layer_sends],
        [acc, bias_mid[:, None], down_fine],
        [links, slot],
        [pltpu.VMEM((6, C1 // 2, 128), f32)],
        [arrived],
        [conv_mid],
        far=2,
        sends=6,
    )
    acc = coarse_conv(second, conv_res)
    pools = swap(faces, send, spill)
    refined, coarse = call(
        refined_kernel,
        [(C2, 512), (MEMBERS, TOKB, C2)],
        [acc, second],
        [final],
        [pltpu.VMEM(layer, f32)],
        pools,
        [conv_res],
    )
    everyone = along("brick", coarse)
    joined, faces, send, spill = call(
        attention_kernel,
        [(C2, 512), layer, *layer_sends],
        [everyone, refined, down_mid, w_query, w_key, w_value, w_out, up_mid],
        [logit_scale, labels[0], me, slot],
        far=2,
        sends=6,
    )
    acc = coarse_conv(joined, conv_dec)
    pools = swap(faces, send, spill)
    mix, faces, send, spill = call(
        decoded_kernel,
        [(C1, S**3), fine_layer, *fine_sends],
        [acc],
        [final, slot],
        [pltpu.VMEM(layer, f32)],
        pools,
        [conv_dec, up_fine, first],
        far=2,
        sends=6,
    )
    acc = fine_conv(mix, conv_out)
    pools = swap(faces, send, spill)
    (result,) = call(
        fine_last_kernel,
        [(C1, S**3)],
        [],
        [final],
        [pltpu.VMEM(fine_layer, f32)],
        pools,
        [acc, conv_out],
    )
    return result[None]


def solution(mesh):
    in_specs = (
        P(("grp", "brick"), None, None),
        P(("grp", "brick"), None),
        P("grp", None),
    ) + (P(),) * 16
    out_specs = P(("grp", "brick"), None, None)
    return jax.shard_map(
        per_device, mesh=mesh, in_specs=in_specs, out_specs=out_specs, check_vma=False
    )
```

```python
import jax
import jax.numpy as jnp
from jax import lax
from jax.experimental import pallas as pl
from jax.experimental.pallas import tpu as pltpu
from jax.sharding import PartitionSpec as P

S = 16
C1 = 64
C2 = 128
C3 = 256
HEADS = 4
HDIM = 64
TOKB = 64
BRICKS = 128
GROUPS = 8
MEMBERS = 16
SLOTS_B = 2
SLOTS_G = 3
FROM_B = 6
FROM_X = FROM_B + MEMBERS * SLOTS_B
FROM_G = FROM_X + MEMBERS
FROM_END = FROM_G + GROUPS * SLOTS_G
EPSILON = 1e-06
ALL = ("grp", "brick")

f32 = jnp.float32
bf16 = jnp.bfloat16


def split(v):
    hi = v.astype(bf16)
    return hi, (v - hi.astype(f32)).astype(bf16)


def mm(a, b, nt=False):
    return lax.dot_general(
        a, b, (((1,), (1 if nt else 0,)), ((), ())), preferred_element_type=f32
    )


def dot3(a, b, nt=False):
    rows = a.shape[0]
    ah, al = split(a)
    bh, bl = split(b)
    both = mm(jnp.concatenate([ah, al], axis=0), bh, nt)
    return both[:rows] + both[rows:] + mm(ah, bl, nt)


def dot2(a, selector, nt=False):
    rows = a.shape[0]
    ah, al = split(a)
    both = mm(jnp.concatenate([ah, al], axis=0), selector, nt)
    return both[:rows] + both[rows:]


def iota(shape, dim):
    return lax.broadcasted_iota(jnp.int32, shape, dim)


def as01(mask):
    return jnp.where(mask, 1.0, 0.0).astype(bf16)


def silu(v):
    return v / (1.0 + jnp.exp(-v))


def lane_roll(v, shift):
    amount = shift % v.shape[1]
    return v if amount == 0 else pltpu.roll(v, amount, 1)


def in_range(index, edge):
    return (index >= 0) & (index < edge)


def face_taps(face):
    side = 2 * (face % 2)
    if face < 2:
        return [9 * side + 3 * a + b for a in range(3) for b in range(3)]
    if face < 4:
        return [9 * a + 3 * side + b for a in range(3) for b in range(3)]
    return [9 * a + 3 * b + side for a in range(3) for b in range(3)]


def tap_columns(w_ref, taps, channels):
    runs = []
    for t in taps:
        if runs and runs[-1][1] == t:
            runs[-1][1] = t + 1
        else:
            runs.append([t, t + 1])
    pieces = [w_ref[:, lo * channels : hi * channels] for lo, hi in runs]
    return pieces[0] if len(pieces) == 1 else jnp.concatenate(pieces, axis=1)


def coarse_edges():
    row = iota((384, 512), 0)
    col = iota((384, 512), 1)
    pair = row >> 7
    edge = ((row >> 6) & 1) * 7
    a = (row >> 3) & 7
    b = row & 7
    x = col >> 6
    y = (col >> 3) & 7
    z = col & 7
    along = jnp.where(pair == 0, x, jnp.where(pair == 1, y, z))
    first = jnp.where(pair == 0, y, x)
    last = jnp.where(pair == 2, y, z)
    return as01((along == edge) & (first == a) & (last == b))


def fine_sides():
    row = iota((256, 256), 0)
    col = iota((256, 256), 1)
    edge = (row >> 7) * 15
    return as01(((col & 15) == edge) & ((col >> 4) == (row & 15)))


def fine_sides_t():
    row = iota((256, 256), 0)
    col = iota((256, 256), 1)
    edge = (col >> 7) * 15
    return as01(((row & 15) == edge) & ((row >> 4) == (col & 15)))


class Late:
    def __init__(self, far_ref, near_ref, sem):
        self.near_ref = near_ref
        self.copy = pltpu.make_async_copy(far_ref, near_ref, sem)
        self.copy.start()
        self.here = False

    def __getitem__(self, index):
        if not self.here:
            self.copy.wait()
            self.here = True
        return self.near_ref[index]


def late_copies(far_refs, near_refs, sems):
    return [
        Late(far, near, sems.at[n]) for n, (far, near) in enumerate(zip(far_refs, near_refs))
    ]


def send_faces(faces_ref, slot_ref, send_refs, sems):
    def each(act):
        for face in range(6):
            slot = slot_ref[face]
            base = 0
            for send_ref in send_refs:
                count = send_ref.shape[0]
                inside = (slot >= base) & (slot < base + count)

                @pl.when(inside)
                def _():
                    act(
                        pltpu.make_async_copy(
                            faces_ref.at[face], send_ref.at[slot - base], sems.at[face]
                        )
                    )

                base += count

    each(lambda copy: copy.start())
    each(lambda copy: copy.wait())


def fetch_halo(pools, bounds, index_ref, halo_ref, sems):
    def each(act):
        for face in range(6):
            source = index_ref[face]
            for pool, low, high in zip(pools, bounds[:-1], bounds[1:]):

                @pl.when((source >= low) & (source < high))
                def _():
                    act(
                        pltpu.make_async_copy(
                            pool.at[source - low], halo_ref.at[face], sems.at[face]
                        )
                    )

    each(lambda copy: copy.start())
    for face in range(6):

        @pl.when(index_ref[face] < 0)
        def _():
            halo_ref[face] = jnp.zeros(halo_ref.shape[1:], f32)

    return lambda: each(lambda copy: copy.wait())


BOUNDS = [FROM_B, FROM_X, FROM_G, FROM_END]


def coarse_faces(v, edges, faces_ref):
    rows = v.shape[0] // 2
    picked = dot2(v, edges, nt=True)
    low = iota((rows, 128), 1) < 64
    for pair in range(3):
        block = picked[:, pair * 128 : (pair + 1) * 128]
        top = block[:rows]
        bottom = block[rows:]
        faces_ref[2 * pair] = jnp.where(low, top, pltpu.roll(bottom, 64, 1))
        faces_ref[2 * pair + 1] = jnp.where(low, pltpu.roll(top, 64, 1), bottom)


def fine_faces(v_ref, faces_ref):
    faces_ref[0] = v_ref[:, 0:256]
    faces_ref[1] = v_ref[:, 3840:4096]
    sides = fine_sides_t()
    at_x = iota((C1, 128), 1) >> 4
    for half in range(2):
        found = [None] * 4
        for k in range(8):
            start = (half * 8 + k) * 256
            part = v_ref[:, start : start + 256]
            near = dot2(part, sides)
            new = [
                lane_roll(part[:, :128], 16 * k),
                lane_roll(part[:, 128:], 16 * k - 112),
                near[:, :128],
                near[:, 128:],
            ]
            if k == 0:
                found = new
            else:
                found = [jnp.where(at_x == k, n, o) for n, o in zip(new, found)]
        for kind in range(4):
            faces_ref[2 + kind, :, half * 128 : (half + 1) * 128] = found[kind]


def route_kernel(all_ref, table_ref, me_ref, slot_ref, relay_ref, final_ref, level_ref):
    g = me_ref[0]
    b = me_ref[1]
    me = g * MEMBERS + b
    here = all_ref[...]
    brick = iota((BRICKS, 128), 0)
    same_b = jnp.zeros((BRICKS, 128), f32)
    same_g = jnp.zeros((BRICKS, 128), f32)
    for back in range(1, 6):
        there = pltpu.roll(here, back, 1)
        known = there >= 0
        same_b += jnp.where(known & ((there & 15) == (here & 15)), 1.0, 0.0)
        same_g += jnp.where(known & ((there >> 4) == (here >> 4)), 1.0, 0.0)
    same_b = jnp.where((here >= 0) & ((here & 15) != (brick & 15)), same_b, 0.0)
    same_g = jnp.where((here >= 0) & ((here >> 4) != (brick >> 4)), same_g, 0.0)
    most_b = jnp.max(same_b).astype(jnp.int32)
    most_g = jnp.max(same_g).astype(jnp.int32)
    crowded = (most_b > SLOTS_B) | (most_g >= SLOTS_G)
    level = jnp.where(crowded, 2, jnp.where(most_b == SLOTS_B, 1, 0))
    level_ref[0] = level

    def rank_b(i, face, member):
        count = jnp.int32(0)
        for other in range(5):
            j = table_ref[i, other]
            hit = (j >= 0) & ((j & 15) == member) & (other < face)
            count = count + jnp.where(hit, 1, 0)
        return count

    def rank_g(j, face, group):
        count = jnp.int32(0)
        for other in range(face):
            i = table_ref[j, other]
            hit = (i >= 0) & ((i >> 4) == group)
            count = count + jnp.where(hit, 1, 0)
        return count

    def slot_b(member, rank):
        low = member * SLOTS_B + jnp.minimum(rank, SLOTS_B - 1)
        return jnp.where(rank < SLOTS_B, low, MEMBERS * SLOTS_B + member)

    for face in range(6):
        j = table_ref[me, face]
        member = j & 15
        rank = rank_b(me, face, member)
        fine = (j >= 0) & (member != b) & (rank <= SLOTS_B)
        slot_ref[face] = jnp.where(fine, slot_b(member, rank), -1)
    for slot in range(GROUPS * SLOTS_G):
        relay_ref[slot] = jnp.int32(-1)

    def relay_to(group, carry):
        j = group * MEMBERS + b
        for face in range(6):
            i = table_ref[j, face]
            mine = (i >= 0) & ((i >> 4) == g) & (group != g)
            safe = jnp.maximum(i, 0)
            rank = rank_g(j, face, g)
            first = rank_b(safe, face ^ 1, b)
            member = safe & 15
            source = jnp.where(member == b, face ^ 1, FROM_B + slot_b(member, first))
            fits = mine & (rank < SLOTS_G) & ((member == b) | (first <= SLOTS_B))

            @pl.when(fits)
            def _():
                relay_ref[group * SLOTS_G + rank] = source

        return carry

    lax.fori_loop(0, GROUPS, relay_to, 0)
    for face in range(6):
        i = table_ref[me, face]
        safe = jnp.maximum(i, 0)
        first = rank_b(safe, face ^ 1, b)
        group = safe >> 4
        rank = jnp.minimum(rank_g(me, face, group), SLOTS_G - 1)
        source = jnp.where(
            group == g,
            FROM_B + slot_b(safe & 15, first),
            FROM_G + group * SLOTS_G + rank,
        )
        source = jnp.where(level == 2, FROM_X + face, source)
        final_ref[face] = jnp.where(i >= 0, source, -1)


def relay_kernel(faces_ref, recv_ref, more_ref, index_ref, out_ref, sems):
    def each(act):
        def one(slot, carry):
            source = index_ref[slot]
            starts = [0, FROM_B, FROM_X, FROM_G]
            for pool, low, high in zip(
                (faces_ref, recv_ref, more_ref), starts[:-1], starts[1:]
            ):

                @pl.when((source >= low) & (source < high))
                def _():
                    act(
                        pltpu.make_async_copy(
                            pool.at[source - low], out_ref.at[slot], sems.at[slot]
                        )
                    )

            return carry

        lax.fori_loop(0, GROUPS * SLOTS_G, one, 0)

    each(lambda copy: copy.start())
    each(lambda copy: copy.wait())


def fine_face_kernel(v_ref, faces_ref):
    fine_faces(v_ref, faces_ref)


def pack_kernel(faces_ref, slot_ref, send_ref, spill_ref, sems):
    send_faces(faces_ref, slot_ref, [send_ref, spill_ref], sems)


def split_weights(w_ref, stacked_ref):
    rows = w_ref.shape[0]
    hi, lo = split(w_ref[...])
    stacked_ref[0:rows, :] = hi
    stacked_ref[rows : 2 * rows, :] = lo


def fine_conv_kernel(v_ref, w_ref, out_ref, hi_ref, lo_ref, stacked_ref):
    split_weights(w_ref, stacked_ref)
    for ref in (hi_ref, lo_ref):
        ref[:, 0:256] = jnp.zeros((576, 256), bf16)
        ref[:, 4352:4608] = jnp.zeros((576, 256), bf16)
    lane = iota((C1, 256), 1)
    y = lane >> 4
    z = lane & 15

    def plane(x, carry):
        part = v_ref[:, pl.ds(pl.multiple_of(x * 256, 256), 256)]
        for tap in range(9):
            dy, dz = tap // 3 - 1, tap % 3 - 1
            moved = lane_roll(part, -(16 * dy + dz))
            keep = in_range(y + dy, S) & in_range(z + dz, S)
            hi, lo = split(jnp.where(keep, moved, 0.0))
            at = pl.ds(pl.multiple_of(x * 256 + 256, 256), 256)
            hi_ref[tap * C1 : (tap + 1) * C1, at] = hi
            lo_ref[tap * C1 : (tap + 1) * C1, at] = lo
        return carry

    lax.fori_loop(0, S, plane, 0)

    def block(n, carry):
        def gathered(ref):
            return jnp.concatenate(
                [
                    ref[:, pl.ds(pl.multiple_of(n * 256 + dx * 256, 256), 256)]
                    for dx in range(3)
                ],
                axis=0,
            )

        both = mm(stacked_ref[...], gathered(hi_ref))
        low = mm(stacked_ref[0:C1, :], gathered(lo_ref))
        at = pl.ds(pl.multiple_of(n * 256, 256), 256)
        out_ref[:, at] = both[:C1] + both[C1:] + low
        return carry

    lax.fori_loop(0, S, block, 0)


def fine_halo(acc_ref, halo_ref, w_ref, out_ref):
    lane = iota((C1, 256), 1)
    a = lane >> 4
    b = lane & 15
    sheets = []
    for face in range(6):
        layer = halo_ref[face]
        his, los = [], []
        for tap in range(9):
            da, db = tap // 3 - 1, tap % 3 - 1
            keep = in_range(a + da, S) & in_range(b + db, S)
            moved = lane_roll(layer, -(16 * da + db))
            hi, lo = split(jnp.where(keep, moved, 0.0))
            his.append(hi)
            los.append(lo)
        wh, wl = split(tap_columns(w_ref, face_taps(face), C1))
        both = mm(jnp.concatenate([wh, wl], axis=0), jnp.concatenate(his, axis=0))
        low = mm(wh, jnp.concatenate(los, axis=0))
        sheets.append(both[:C1] + both[C1:] + low)
    sides = fine_sides()
    at_x = (iota((2 * C1, 256), 1) >> 4) & 7
    lane = iota((C1, 128), 1)
    for half in range(2):
        at = slice(half * 128, (half + 1) * 128)
        near = jnp.concatenate([sheets[4][:, at], sheets[5][:, at]], axis=1)
        hi, lo = split(near)
        spread = jnp.concatenate([hi, lo], axis=0)
        for k in range(8):
            x = half * 8 + k
            both = mm(spread * as01(at_x == k), sides)
            start = x * 256
            total = acc_ref[:, start : start + 256] + both[:C1] + both[C1:]
            low = lane_roll(sheets[2][:, at], -16 * k)
            high = lane_roll(sheets[3][:, at], 112 - 16 * k)
            ends = jnp.concatenate(
                [jnp.where(lane < 16, low, 0.0), jnp.where(lane >= 112, high, 0.0)], axis=1
            )
            total = total + ends
            if x == 0:
                total = total + sheets[0]
            if x == S - 1:
                total = total + sheets[1]
            out_ref[:, start : start + 256] = total


def fine_last_kernel(
    recv_ref,
    more_ref,
    relayed_ref,
    acc_far,
    w_far,
    final_ref,
    out_ref,
    halo_ref,
    acc_near,
    w_near,
    sems,
    halo_sems,
):
    arrive = fetch_halo([recv_ref, more_ref, relayed_ref], BOUNDS, final_ref, halo_ref, halo_sems)
    acc_ref, w_ref = late_copies([acc_far, w_far], [acc_near, w_near], sems)
    arrive()
    fine_halo(acc_ref, halo_ref, w_ref, out_ref)


def fine_first_kernel(
    bias_ref,
    down_ref,
    recv_ref,
    more_ref,
    relayed_ref,
    acc_far,
    w_far,
    final_ref,
    links_ref,
    mid_ref,
    first_far,
    send_ref,
    halo_ref,
    first_ref,
    faces_ref,
    acc_near,
    w_near,
    sems,
    halo_sems,
    send_sems,
):
    arrive = fetch_halo([recv_ref, more_ref, relayed_ref], BOUNDS, final_ref, halo_ref, halo_sems)
    acc_ref, w_ref = late_copies([acc_far, w_far], [acc_near, w_near], sems)
    arrive()
    fine_halo(acc_ref, halo_ref, w_ref, first_ref)
    first_ref[...] = silu(first_ref[...] + bias_ref[...])
    keep = pltpu.make_async_copy(first_ref, first_far, sems.at[0])
    keep.start()
    row = iota((512, 128), 0)
    col = iota((512, 128), 1)
    target = (row >> 8) * 64 + ((row >> 5) & 7) * 8 + ((row >> 1) & 7)
    pool = jnp.where(target == col, 0.125, 0.0).astype(bf16)
    parts = []
    for quad in range(4):
        planes = [
            first_ref[:, (4 * quad + k) * 256 : (4 * quad + k + 1) * 256] for k in range(4)
        ]
        pair = jnp.concatenate([planes[0] + planes[1], planes[2] + planes[3]], axis=1)
        parts.append(dot2(pair, pool))
    shrunk = jnp.concatenate(parts, axis=1)
    mid_ref[...] = dot3(down_ref[...], shrunk)
    coarse_faces(shrunk, coarse_edges(), faces_ref)
    send_faces(faces_ref, links_ref, [send_ref], send_sems)
    keep.wait()


def coarse_conv_kernel(v_ref, w_ref, out_ref, hi_ref, lo_ref, stacked_ref):
    split_weights(w_ref, stacked_ref)
    lane = iota((16, 512), 1)
    x = lane >> 6
    y = (lane >> 3) & 7
    z = lane & 7

    def chunk(n, carry):
        part = v_ref[pl.ds(pl.multiple_of(n * 16, 16), 16), :]
        for tap in range(27):
            dx, dy, dz = tap // 9 - 1, tap // 3 % 3 - 1, tap % 3 - 1
            keep = in_range(x + dx, 8) & in_range(y + dy, 8) & in_range(z + dz, 8)
            moved = lane_roll(part, -(64 * dx + 8 * dy + dz))
            hi, lo = split(jnp.where(keep, moved, 0.0))
            at = pl.ds(pl.multiple_of(tap * C2 + n * 16, 16), 16)
            hi_ref[at, :] = hi
            lo_ref[at, :] = lo
        return carry

    lax.fori_loop(0, C2 // 16, chunk, 0)

    out_ref[...] = jnp.zeros((C2, 512), f32)

    def block(triple, carry):
        at = pl.ds(pl.multiple_of(triple * 3 * C2, 128), 3 * C2)
        both = mm(stacked_ref[:, at], hi_ref[at, :])
        low = mm(stacked_ref[0:C2, at], lo_ref[at, :])
        out_ref[...] += both[:C2] + both[C2:] + low
        return carry

    lax.fori_loop(0, 9, block, 0)


def coarse_halo(acc_ref, halo_ref, w_ref, edges, down=None):
    rows = halo_ref.shape[1]
    low_lane = iota((rows, 128), 1) < 64
    lane = iota((C2, 128), 1)
    a = (lane >> 3) & 7
    b = lane & 7
    sheets = []
    for pair in range(3):
        even = halo_ref[2 * pair]
        odd = halo_ref[2 * pair + 1]
        top = jnp.where(low_lane, even, pltpu.roll(odd, 64, 1))
        bottom = jnp.where(low_lane, pltpu.roll(even, 64, 1), odd)
        layer = jnp.concatenate([top, bottom], axis=0)
        if down is not None:
            layer = dot3(down, layer)
        his, los = [], []
        for tap in range(9):
            da, db = tap // 3 - 1, tap % 3 - 1
            keep = in_range(a + da, 8) & in_range(b + db, 8)
            moved = lane_roll(layer, -(8 * da + db))
            hi, lo = split(jnp.where(keep, moved, 0.0))
            his.append(hi)
            los.append(lo)
        eh, el = split(tap_columns(w_ref, face_taps(2 * pair), C2))
        oh, ol = split(tap_columns(w_ref, face_taps(2 * pair + 1), C2))
        both = mm(jnp.concatenate([eh, el, oh, ol], axis=0), jnp.concatenate(his, axis=0))
        low = mm(jnp.concatenate([eh, oh], axis=0), jnp.concatenate(los, axis=0))
        even_sum = both[0:C2] + both[C2 : 2 * C2] + low[0:C2]
        odd_sum = both[2 * C2 : 3 * C2] + both[3 * C2 :] + low[C2:]
        sheets.append(jnp.where(lane < 64, even_sum, odd_sum))
    return acc_ref[...] + dot2(jnp.concatenate(sheets, axis=1), edges)


def second_kernel(
    acc_ref,
    bias_ref,
    down_ref,
    arrived_ref,
    w_far,
    links_ref,
    slot_ref,
    second_ref,
    faces_ref,
    send_ref,
    spill_ref,
    halo_ref,
    w_near,
    sems,
    halo_sems,
    send_sems,
):
    arrive = fetch_halo([arrived_ref], [0, BRICKS], links_ref, halo_ref, halo_sems)
    (w_ref,) = late_copies([w_far], [w_near], sems)
    arrive()
    edges = coarse_edges()
    summed = coarse_halo(acc_ref, halo_ref, w_ref, edges, down_ref[...])
    second = silu(summed + bias_ref[...])
    second_ref[...] = second
    coarse_faces(second, edges, faces_ref)
    send_faces(faces_ref, slot_ref, [send_ref, spill_ref], send_sems)


def pool_rows(scale):
    row = iota((64, 512), 0)
    col = iota((64, 512), 1)
    target = (col >> 7) * 16 + ((col >> 4) & 3) * 4 + ((col >> 1) & 3)
    return jnp.where(target == row, scale, 0.0).astype(bf16)


def refined_kernel(
    acc_ref,
    second_ref,
    recv_ref,
    more_ref,
    relayed_ref,
    w_far,
    final_ref,
    refined_ref,
    coarse_ref,
    halo_ref,
    w_near,
    sems,
    halo_sems,
):
    arrive = fetch_halo([recv_ref, more_ref, relayed_ref], BOUNDS, final_ref, halo_ref, halo_sems)
    (w_ref,) = late_copies([w_far], [w_near], sems)
    arrive()
    summed = coarse_halo(acc_ref, halo_ref, w_ref, coarse_edges())
    refined = second_ref[...] + silu(summed)
    refined_ref[...] = refined
    pool = pool_rows(0.125)
    hi, lo = split(refined)
    coarse = mm(pool, hi, nt=True) + mm(pool, lo, nt=True)
    for member in range(MEMBERS):
        coarse_ref[member] = coarse


def attention_kernel(
    all_ref,
    refined_ref,
    down_ref,
    wq_ref,
    wk_ref,
    wv_ref,
    wo_ref,
    up_ref,
    scale_ref,
    labels_ref,
    me_ref,
    slot_ref,
    joined_ref,
    faces_ref,
    send_ref,
    spill_ref,
    send_sems,
):
    head_of = iota((C3, C3), 1) >> 6
    head_mean = jnp.where((iota((C3, C3), 0) >> 6) == head_of, 1.0 / HDIM, 0.0).astype(bf16)

    def normed(v):
        return v * lax.rsqrt(jnp.mean(v * v, axis=-1, keepdims=True) + EPSILON)

    def head_normed(v):
        return v * lax.rsqrt(dot2(v * v, head_mean) + EPSILON)

    tokens = dot3(all_ref[me_ref[1]], down_ref[...], nt=True)
    query = head_normed(dot3(normed(tokens), wq_ref[...]))
    gathered = all_ref[...].reshape(MEMBERS * TOKB, C2)
    everyone = normed(dot3(gathered, down_ref[...], nt=True))
    keys = head_normed(dot3(everyone, wk_ref[...]))
    values = dot3(everyone, wv_ref[...])
    lane_head = iota((TOKB, C3), 1) >> 6
    stacked = jnp.concatenate(
        [
            jnp.where(lane_head == h, query, 0.0) * (scale_ref[h] * (HDIM**-0.5))
            for h in range(HEADS)
        ],
        axis=0,
    )
    logits = dot3(stacked, keys, nt=True)
    brick_of = iota((1, MEMBERS * TOKB), 1) >> 6
    key_label = jnp.zeros((1, MEMBERS * TOKB), jnp.int32)
    for member in range(MEMBERS):
        key_label = jnp.where(brick_of == member, labels_ref[member], key_label)
    allowed = key_label == labels_ref[me_ref[1]]
    logits = jnp.where(allowed, logits, -1e30)
    peak = jnp.max(logits, axis=-1, keepdims=True)
    weight = jnp.where(allowed, jnp.exp(logits - peak), 0.0)
    total = jnp.sum(weight, axis=-1, keepdims=True)
    heads = dot3(weight, values) / total
    attended = jnp.zeros((TOKB, C3), f32)
    for h in range(HEADS):
        attended = jnp.where(lane_head == h, heads[h * TOKB : (h + 1) * TOKB], attended)
    mixed = tokens + dot3(attended, wo_ref[...])
    lifted = dot3(up_ref[...], mixed, nt=True)
    joined = refined_ref[...] + dot2(lifted, pool_rows(1.0))
    joined_ref[...] = joined
    coarse_faces(joined, coarse_edges(), faces_ref)
    send_faces(faces_ref, slot_ref, [send_ref, spill_ref], send_sems)


def decoded_kernel(
    acc_ref,
    recv_ref,
    more_ref,
    relayed_ref,
    w_far,
    up_far,
    first_far,
    final_ref,
    slot_ref,
    mix_ref,
    faces_ref,
    send_ref,
    spill_ref,
    halo_ref,
    w_near,
    up_near,
    first_near,
    sems,
    halo_sems,
    send_sems,
):
    arrive = fetch_halo([recv_ref, more_ref, relayed_ref], BOUNDS, final_ref, halo_ref, halo_sems)
    w_ref, up_ref, first_ref = late_copies(
        [w_far, up_far, first_far], [w_near, up_near, first_near], sems
    )
    arrive()
    decoded = silu(coarse_halo(acc_ref, halo_ref, w_ref, coarse_edges()))
    dropped = dot3(up_ref[...], decoded)
    row = iota((128, 1024), 0)
    col = iota((128, 1024), 1)
    source = (col >> 9) * 64 + ((col >> 5) & 7) * 8 + ((col >> 1) & 7)
    widen = as01(source == row)
    for quad in range(4):
        wide = dot2(dropped[:, quad * 128 : (quad + 1) * 128], widen)
        at = slice(quad * 1024, (quad + 1) * 1024)
        mix_ref[:, at] = silu(first_ref[:, at] + wide)
    fine_faces(mix_ref, faces_ref)
    send_faces(faces_ref, slot_ref, [send_ref, spill_ref], send_sems)


VMEM = pl.BlockSpec(memory_space=pltpu.VMEM)
SMEM = pl.BlockSpec(memory_space=pltpu.SMEM)
FAR = pl.BlockSpec(memory_space=pl.ANY)


def grant(mib):
    return pltpu.CompilerParams(vmem_limit_bytes=mib << 20)


def call(kernel, outs, args=(), scalars=(), scratch=(), pools=(), late=(), far=0, sends=0, mib=None):
    near = len(outs) - far
    copies = [pltpu.VMEM(v.shape, v.dtype) for v in late]
    sems = [pltpu.SemaphoreType.DMA((len(late),))] if late else []
    if pools:
        sems.append(pltpu.SemaphoreType.DMA((6,)))
    if sends:
        sems.append(pltpu.SemaphoreType.DMA((sends,)))
    return pl.pallas_call(
        kernel,
        out_shape=[jax.ShapeDtypeStruct(o, f32) for o in outs],
        in_specs=[VMEM] * len(args) + [FAR] * (len(pools) + len(late)) + [SMEM] * len(scalars),
        out_specs=[VMEM] * near + [FAR] * far,
        scratch_shapes=[*scratch, *copies, *sems],
        compiler_params=grant(mib) if mib else None,
    )(*args, *pools, *late, *scalars)


def route(rows, me):
    sizes = [6, GROUPS * SLOTS_G, 6, 1]
    return pl.pallas_call(
        route_kernel,
        out_shape=[jax.ShapeDtypeStruct((n,), jnp.int32) for n in sizes],
        in_specs=[VMEM, SMEM, SMEM],
        out_specs=[SMEM] * len(sizes),
        compiler_params=grant(4),
    )(rows, rows, me)


def table_kernel(links_ref, out_ref):
    lane = iota((BRICKS, 128), 1)
    row = jnp.full((BRICKS, 128), -1, jnp.int32)
    for face in range(6):
        row = jnp.where(lane == face, links_ref[face], row)
    out_ref[...] = row


def table_of(links):
    return pl.pallas_call(
        table_kernel,
        out_shape=jax.ShapeDtypeStruct((BRICKS, 128), jnp.int32),
        in_specs=[SMEM],
        out_specs=VMEM,
        compiler_params=grant(4),
    )(links)


def dense_halo(faces, links):
    owners = lax.broadcasted_iota(jnp.int32, (BRICKS, 6), 0)
    chosen = links[None, :] == owners
    parcel = jnp.zeros((BRICKS, *faces.shape[1:]), f32)
    for face in range(6):
        parcel = jnp.where(chosen[:, face, None, None], faces[face][None], parcel)
    arrived = lax.all_to_all(parcel, ALL, 0, 0, tiled=True)
    halos = []
    for face in range(6):
        layer = lax.dynamic_index_in_dim(
            arrived, jnp.maximum(links[face], 0), 0, keepdims=False
        )
        halos.append(jnp.where(links[face] >= 0, layer, 0.0))
    return jnp.stack(halos)


def along(axis, slots):
    count = lax.axis_size(axis)
    rows = slots.shape[0] // count * slots.shape[1]
    blocks = slots.reshape(count, rows, slots.shape[2])
    return lax.all_to_all(blocks, axis, 0, 0, tiled=True).reshape(slots.shape)


def exchange(faces, send, spill, relay, links, level):
    layer = faces.shape[1:]

    def nothing(operands):
        return jnp.zeros((MEMBERS, *layer), f32)

    def third(operands):
        return along("brick", operands[1])

    def dense(operands):
        halo = dense_halo(operands[0], links)
        return jnp.concatenate([halo, jnp.zeros((MEMBERS - 6, *layer), f32)])

    recv = along("brick", send)
    more = lax.switch(level, [nothing, third, dense], (faces, spill))
    (onward,) = call(
        relay_kernel,
        [(GROUPS * SLOTS_G, *layer)],
        [faces, recv, more],
        [relay],
        far=1,
        sends=GROUPS * SLOTS_G,
        mib=8,
    )
    return [recv, more, along("grp", onward)]


def per_device(
    noisy,
    neighbours,
    labels,
    conv_in,
    bias_in,
    down_fine,
    conv_mid,
    bias_mid,
    conv_res,
    conv_dec,
    down_mid,
    w_query,
    w_key,
    w_value,
    w_out,
    logit_scale,
    up_mid,
    up_fine,
    conv_out,
):
    links = neighbours[0]
    me = jnp.stack([lax.axis_index("grp"), lax.axis_index("brick")]).astype(jnp.int32)
    rows = lax.all_to_all(table_of(links), ALL, 0, 0, tiled=True)
    slot, relay, final, level = route(rows, me)
    level = level[0]

    def swap(faces, send, spill):
        return exchange(faces, send, spill, relay, links, level)

    fine_layer = (6, C1, 256)
    fine_sends = [(MEMBERS * SLOTS_B, C1, 256), (MEMBERS, C1, 256)]
    layer = (6, C2 // 2, 128)
    layer_sends = [(MEMBERS * SLOTS_B, C2 // 2, 128), (MEMBERS, C2 // 2, 128)]

    def fine_conv(v, w):
        return call(
            fine_conv_kernel,
            [(C1, S**3)],
            [v, w],
            scratch=[
                pltpu.VMEM((576, 4608), bf16),
                pltpu.VMEM((576, 4608), bf16),
                pltpu.VMEM((2 * C1, 27 * C1), bf16),
            ],
        )[0]

    def coarse_conv(v, w):
        return call(
            coarse_conv_kernel,
            [(C2, 512)],
            [v, w],
            scratch=[
                pltpu.VMEM((27 * C2, 512), bf16),
                pltpu.VMEM((27 * C2, 512), bf16),
                pltpu.VMEM((2 * C2, 27 * C2), bf16),
            ],
        )[0]

    fine_in = noisy[0]
    (faces,) = call(fine_face_kernel, [fine_layer], [fine_in])
    send, spill = call(
        pack_kernel, fine_sends, [faces], [slot], far=2, sends=6, mib=8
    )
    acc = fine_conv(fine_in, conv_in)
    pools = swap(faces, send, spill)
    mid, first, send = call(
        fine_first_kernel,
        [(C2, 512), (C1, S**3), (BRICKS, C1 // 2, 128)],
        [bias_in[:, None], down_fine],
        [final, links],
        [
            pltpu.VMEM(fine_layer, f32),
            pltpu.VMEM((C1, S**3), f32),
            pltpu.VMEM((6, C1 // 2, 128), f32),
        ],
        pools,
        [acc, conv_in],
        far=2,
        sends=6,
    )
    acc = coarse_conv(mid, conv_mid)
    arrived = lax.all_to_all(send, ALL, 0, 0, tiled=True)
    second, faces, send, spill = call(
        second_kernel,
        [(C2, 512), layer, *layer_sends],
        [acc, bias_mid[:, None], down_fine],
        [links, slot],
        [pltpu.VMEM((6, C1 // 2, 128), f32)],
        [arrived],
        [conv_mid],
        far=2,
        sends=6,
    )
    acc = coarse_conv(second, conv_res)
    pools = swap(faces, send, spill)
    refined, coarse = call(
        refined_kernel,
        [(C2, 512), (MEMBERS, TOKB, C2)],
        [acc, second],
        [final],
        [pltpu.VMEM(layer, f32)],
        pools,
        [conv_res],
    )
    everyone = along("brick", coarse)
    joined, faces, send, spill = call(
        attention_kernel,
        [(C2, 512), layer, *layer_sends],
        [everyone, refined, down_mid, w_query, w_key, w_value, w_out, up_mid],
        [logit_scale, labels[0], me, slot],
        far=2,
        sends=6,
    )
    acc = coarse_conv(joined, conv_dec)
    pools = swap(faces, send, spill)
    mix, faces, send, spill = call(
        decoded_kernel,
        [(C1, S**3), fine_layer, *fine_sends],
        [acc],
        [final, slot],
        [pltpu.VMEM(layer, f32)],
        pools,
        [conv_dec, up_fine, first],
        far=2,
        sends=6,
    )
    acc = fine_conv(mix, conv_out)
    pools = swap(faces, send, spill)
    (result,) = call(
        fine_last_kernel,
        [(C1, S**3)],
        [],
        [final],
        [pltpu.VMEM(fine_layer, f32)],
        pools,
        [acc, conv_out],
    )
    return result[None]


def solution(mesh):
    in_specs = (
        P(("grp", "brick"), None, None),
        P(("grp", "brick"), None),
        P("grp", None),
    ) + (P(),) * 16
    out_specs = P(("grp", "brick"), None, None)
    return jax.shard_map(
        per_device, mesh=mesh, in_specs=in_specs, out_specs=out_specs, check_vma=False
    )
```
